256 devices in a mesh: row: 8 (over z), col: 4 (over y_lo, core), rep: 8 (over x, y_hi).
Axes of the slice: x: 4, y: 4 (y_hi: 2, y_lo: 2; y = y_hi * 2 + y_lo), z: 8, core: 2. Of those that a mesh axis runs over, the one named last changes fastest.
Arguments:
- upstream: float32 [16384, 16384], P('row', ('col', 'rep')), may hold values from -0.046875 to 0.046875
- input_panel: float32 [16384, 1024], P('row', ('col', 'rep')), may hold values from -6 to 6
Outputs:
- panel_grad: float32 [16384, 1024], P('row', ('col', 'rep'))
The draws below stay inside these ranges and needn't reach their ends.
All inputs are finite; a program needn't handle non-finite values.
Results may differ from the reference program's by a relative error of at most 0.000071.
Values sent between devices are 32-bit elements; how exact they have to be, the bound alone decides.
A program may use at most 128 MiB of HBM per device.

```python
import jax
import jax.numpy as jnp
from jax import lax

N = 16384
K = 1024


def block_scale(stream_key, extent, split, least, high):
    def one(dim, parts):
        draws = jax.random.uniform(jax.random.fold_in(jax.random.fold_in(stream_key, 6), dim), (parts,), jnp.float32, least / len(split), high / len(split))
        return jnp.repeat(jnp.exp(draws), extent[dim] // parts).reshape((-1,) + (1,) * (len(extent) - dim - 1))

    level = one(*split[0])
    for cut in split[1:]:
        level = level * one(*cut)
    return level


def scatter_about(key, extent, scale, bound, shards=(), dtype=jnp.bfloat16):
    level = block_scale(key, extent, shards, -0.22, 0.18) if shards else 1.0
    array = jax.random.normal(key, extent, jnp.float32) * scale * level
    return jnp.minimum(jnp.maximum(array, -bound), bound).astype(dtype)


def setup_inputs(seed: int = 0) -> dict:
    streams_of = jax.random.split(jax.random.key(seed), 3)
    upstream = scatter_about(streams_of[0], (N, N), N ** -0.5, 0.046875, ((0, 8), (1, 32)), jnp.float32)
    input_panel = scatter_about(streams_of[1], (N, K), 1.0, 6.0, ((0, 8), (1, 32)), jnp.float32)
    return {"upstream": upstream, "input_panel": input_panel}


def reference(upstream, input_panel):
    precise = lax.Precision.HIGHEST
    lower_tile = jnp.tril(upstream)
    direct = jnp.dot(lower_tile, input_panel, precision=precise, preferred_element_type=jnp.float32)
    mirror = lax.dot_general(lower_tile, input_panel, (((0,), (0,)), ((), ())), precision=precise, preferred_element_type=jnp.float32)
    return direct + mirror
```

```python
import functools

import jax
import jax.numpy as jnp
from jax import lax
from jax.experimental import pallas as pl
from jax.experimental.pallas import tpu as pltpu
from jax.sharding import PartitionSpec as P

MESH = pl.DeviceIdType.MESH
ROWS = 2048
COLS = 512
HALF = ROWS // 2
CHUNKS = 4
WIDE = 256
PIECES = 16
PART = 64
DEPTH = 5
SKEW = 2
AWAY = (0, 3, 1, 2)
EXCHANGE = 22


def at(start, length, step):
    return pl.ds(pl.multiple_of(start, step), length)


def halves(x):
    high = x.astype(jnp.bfloat16)
    return high, (x - high.astype(jnp.float32)).astype(jnp.bfloat16)


def kernel(
    upstream, panel, out,
    gathered, block, upper_sum, upper_in, lower_sum,
    in_partner, in_far, in_near, in_cross_far, in_cross,
    tile, tile_high, tile_low, left_high, left_low, right_high, right_low,
    send_sem, recv_sem, z_send, z_down, z_up, local_sem,
):
    row, col, rep = lax.axis_index("row"), lax.axis_index("col"), lax.axis_index("rep")
    core, x = lax.rem(col, 2), lax.div(rep, 2)
    y = lax.rem(rep, 2) * 2 + lax.div(col, 2)
    me = col * 8 + rep

    def chip(order, first, second):
        dx, dy = (first, second) if order == 0 else (second, first)
        return lax.rem(x + dx, 4), lax.rem(y + dy, 4)

    def number(place, on):
        return (lax.rem(place[1], 2) * 2 + on) * 8 + place[0] * 2 + lax.div(place[1], 2)

    def device(place, on):
        return (row, lax.rem(place[1], 2) * 2 + on, place[0] * 2 + lax.div(place[1], 2))

    low = lax.div(col, 2) * 4 + lax.div(x, 2)
    high = low + 2
    source = jnp.where(core == 0, low, high)
    offset = lax.rem(me, 4) * COLS
    active = row >= source
    root = row == source
    below = row > source
    upward = (core == 1) | (row <= high)
    child_up = ((core == 0) & (row >= low) & (row < high)) | ((core == 1) & (row >= high) & (row < 7))
    child_down = (core == 0) & ((root & (high < 7)) | (row > high + 1))
    depth = jnp.where(upward, row - source, 8 - row)
    above = jnp.where(upward, row - 1, jnp.where(row == 7, low, row + 1))
    up_device = (row + 1, col, rep)
    down_device = (jnp.where(root, 7, row - 1), col, rep)
    above_device = (above, col, rep)
    slot = jnp.where(upward, 0, 1)

    def copy(src, dst, which, to):
        return pltpu.make_async_remote_copy(
            src_ref=src, dst_ref=dst, send_sem=send_sem.at[which], recv_sem=recv_sem.at[which],
            device_id=to, device_id_type=MESH,
        )

    sent = []

    def send(src, dst, which, to):
        one = copy(src, dst, which, to)
        one.start()
        sent.append(one)

    partner = device((x, y), 1 - core)

    def arrived(dst, which):
        copy(dst, dst, which, partner).wait_recv()

    first_cols, second_cols, all_cols = pl.ds(0, HALF), pl.ds(HALF, HALF), pl.ds(0, ROWS)

    def slab(q, place, cols=all_cols):
        return gathered.at[at(q * WIDE + number(place, core) * 8, 8, 8), cols]

    def total(q, place, cols=all_cols):
        return lower_sum.at[at(q * WIDE + number(place, core) * 8, 8, 8), cols]

    def group(ref, q, half, on):
        return ref.at[at(q * WIDE + half * 128 + on * 64, 64, 8), :]

    def gather_own_first(q):
        order, base = q % 2, q * EXCHANGE
        own = panel.at[pl.ds(q * 8, 8), :]
        send(own, slab(q, (x, y)), base + 0, device(chip(order, 1, 0), core))
        send(own, slab(q, (x, y)), base + 1, device(chip(order, 3, 0), core))

    def gather_own_second(q):
        order, base = q % 2, q * EXCHANGE
        own = panel.at[pl.ds(q * 8, 8), :]
        send(own, slab(q, (x, y)), base + 4, device(chip(order, 0, 1), core))
        send(own, slab(q, (x, y)), base + 5, device(chip(order, 0, 3), core))

    def gather_across(q, j):
        order, base = q % 2, q * EXCHANGE + 4 + 2 * j
        piece = slab(q, chip(order, AWAY[j], 0))
        send(piece, piece, base + 0, device(chip(order, 0, 1), core))
        send(piece, piece, base + 1, device(chip(order, 0, 3), core))

    def gather_first(q):
        order, base = q % 2, q * EXCHANGE
        arrived(slab(q, chip(order, 3, 0)), base + 0)
        piece = slab(q, chip(order, 3, 0), first_cols)
        send(piece, piece, base + 2, device(chip(order, 1, 0), core))
        gather_across(q, 1)
        arrived(slab(q, chip(order, 1, 0)), base + 1)
        piece = slab(q, chip(order, 1, 0), second_cols)
        send(piece, piece, base + 3, device(chip(order, 3, 0), core))
        gather_across(q, 2)

    def gather_opposite(q):
        order, base = q % 2, q * EXCHANGE
        arrived(slab(q, chip(order, 2, 0), first_cols), base + 2)
        arrived(slab(q, chip(order, 2, 0), second_cols), base + 3)
        gather_across(q, 3)

    def gather_forward(q, j):
        order, base = q % 2, q * EXCHANGE + 4 + 2 * j
        arrived(slab(q, chip(order, AWAY[j], 3)), base + 0)
        piece = slab(q, chip(order, AWAY[j], 3), first_cols)
        send(piece, piece, base + 8, device(chip(order, 0, 1), core))
        arrived(slab(q, chip(order, AWAY[j], 1)), base + 1)
        piece = slab(q, chip(order, AWAY[j], 1), second_cols)
        send(piece, piece, base + 9, device(chip(order, 0, 3), core))

    def gather_last(q):
        order, base = q % 2, q * EXCHANGE + 12
        for j in range(4):
            arrived(slab(q, chip(order, AWAY[j], 2), first_cols), base + 2 * j)
            arrived(slab(q, chip(order, AWAY[j], 2), second_cols), base + 2 * j + 1)
        for half in range(2):
            piece = group(gathered, q, half, core)
            send(piece, piece, q * EXCHANGE + 20 + half, partner)

    def gather_done(q):
        for half in range(2):
            arrived(group(gathered, q, half, 1 - core), q * EXCHANGE + 20 + half)

    def part(ref, k, more=0):
        return ref.at[at(more + k * PART, PART, PART), :]

    def z_copy(src, k, way, to):
        return pltpu.make_async_remote_copy(
            src_ref=src, dst_ref=part(block, k), send_sem=z_send.at[way * PIECES + k], recv_sem=z_down.at[k],
            device_id=to, device_id_type=MESH,
        )

    def z_start(q):
        @pl.when(root)
        def _():
            def one(i, carry):
                k = q * 4 + i
                src = gathered.at[at(k * PART, PART, PART), at(offset, COLS, COLS)]

                @pl.when(child_up)
                def _():
                    z_copy(src, k, 0, up_device).start()

                @pl.when(child_down)
                def _():
                    z_copy(src, k, 1, down_device).start()

                return carry

            lax.fori_loop(0, 4, one, 0)

    def z_round(step):
        k = step - SKEW * (depth - 1)

        @pl.when(below & (k >= 0) & (k < PIECES))
        def _():
            src = part(block, k)
            z_copy(src, k, 0, up_device).wait_recv()

            @pl.when(child_up)
            def _():
                z_copy(src, k, 0, up_device).start()

            @pl.when(child_down)
            def _():
                z_copy(src, k, 1, down_device).start()

    def sum_copy(k, which):
        return pltpu.make_async_remote_copy(
            src_ref=part(upper_sum, k), dst_ref=part(upper_in, k, which * PIECES * PART),
            send_sem=z_send.at[2 * PIECES + k], recv_sem=z_up.at[which * PIECES + k],
            device_id=above_device, device_id_type=MESH,
        )

    def sum_round(step):
        k = step - SKEW * (DEPTH - depth)

        @pl.when(active & (k >= 0) & (k < PIECES))
        def _():
            for which, there in enumerate((child_up, child_down)):
                @pl.when(there)
                def _():
                    sum_copy(k, which).wait_recv()
                    mine = at(k * PART, PART, PART)
                    other = at(which * PIECES * PART + k * PART, PART, PART)
                    upper_sum[mine, :] = upper_sum[mine, :] + upper_in[other, :]

            @pl.when(below)
            def _():
                sum_copy(k, slot).start()

    def prepare():
        def one(n, carry):
            rows = at(n * 256, 256, 256)
            pltpu.make_async_copy(upstream.at[rows, :], tile.at[rows, :], local_sem.at[n]).wait()
            row_number = row * ROWS + n * 256 + lax.broadcasted_iota(jnp.int32, (256, COLS), 0)
            col_number = me * COLS + lax.broadcasted_iota(jnp.int32, (256, COLS), 1)
            kept = jnp.where(col_number <= row_number, tile[rows, :], 0.0)
            tile_high[rows, :], tile_low[rows, :] = halves(kept)
            return carry

        lax.fori_loop(0, 8, one, 0)

        @pl.when(jnp.logical_not(active))
        def _():
            def clear(n, carry):
                lower_sum[at(n * 64, 64, 64), :] = jnp.zeros((64, ROWS), jnp.float32)
                return carry

            lax.fori_loop(0, 16, clear, 0)

    def product(left_a, left_b, right_a, right_b, dims):
        dot = functools.partial(
            lax.dot_general, dimension_numbers=(dims, ((), ())), preferred_element_type=jnp.float32
        )
        return dot(left_a, right_a) + dot(left_b, right_a) + dot(left_a, right_b)

    def upper(q):
        @pl.when(active)
        def _():
            here = pl.ds(q * WIDE, WIDE)

            def cut(n, carry):
                cols = at(n * 256, 256, 256)
                left_high[:, cols], left_low[:, cols] = halves(gathered[here, cols])
                return carry

            lax.fori_loop(0, 8, cut, 0)

            def one(n, carry):
                cols = at(n * 256, 256, 256)
                upper_sum[here, cols] = product(
                    left_high[...], left_low[...], tile_high[:, cols], tile_low[:, cols], ((1,), (0,))
                )
                return carry

            lax.fori_loop(0, 2, one, 0)

    def lower(q):
        @pl.when(active)
        def _():
            here = pl.ds(q * WIDE, WIDE)

            @pl.when(root)
            def _():
                right_high[...], right_low[...] = halves(gathered[here, at(offset, COLS, COLS)])

            @pl.when(below)
            def _():
                right_high[...], right_low[...] = halves(block[here, :])

            def one(n, carry):
                rows = at(n * 256, 256, 256)
                lower_sum[here, rows] = product(
                    right_high[...], right_low[...], tile_high[rows, :], tile_low[rows, :], ((1,), (1,))
                )
                return carry

            lax.fori_loop(0, 8, one, 0)

    def scatter_partner(q):
        @pl.when(root)
        def _():
            here, cols = pl.ds(q * WIDE, WIDE), at(offset, COLS, COLS)
            lower_sum[here, cols] = lower_sum[here, cols] + upper_sum[here, :]

        for half in range(2):
            send(
                group(lower_sum, q, half, 1 - core), in_partner.at[pl.ds((q * 2 + half) * 64, 64), :],
                (CHUNKS + q) * EXCHANGE + half, partner,
            )

    def scatter_far(q):
        order, base = q % 2, (CHUNKS + q) * EXCHANGE
        for half in range(2):
            came = pl.ds((q * 2 + half) * 64, 64)
            arrived(in_partner.at[came, :], base + half)
            mine = at(q * WIDE + half * 128 + core * 64, 64, 8)
            lower_sum[mine, :] = lower_sum[mine, :] + in_partner[came, :]
        for j in (3, 1, 2, 0):
            to = chip(order, AWAY[j], 2)
            for way, cols in enumerate((first_cols, second_cols)):
                send(
                    total(q, to, cols), in_far.at[pl.ds((q * 8 + 2 * j + way) * 8, 8), :],
                    base + 2 + 2 * j + way, device(chip(order, 0, 1 if way == 0 else 3), core),
                )

    def scatter_near(q):
        order, base = q % 2, (CHUNKS + q) * EXCHANGE
        for j in (3, 1, 2, 0):
            for way, cols in enumerate((first_cols, second_cols)):
                step = 1 if way == 0 else 3
                to = chip(order, AWAY[j], step)
                came = pl.ds((q * 8 + 2 * j + way) * 8, 8)
                arrived(in_far.at[came, :], base + 2 + 2 * j + way)
                mine = at(q * WIDE + number(to, core) * 8, 8, 8)
                lower_sum[mine, cols] = lower_sum[mine, cols] + in_far[came, :]
                send(
                    total(q, to), in_near.at[came, :], base + 10 + 2 * j + way,
                    device(chip(order, 0, step), core),
                )

    def scatter_column(q):
        order, base = q % 2, (CHUNKS + q) * EXCHANGE
        for j in (3, 1, 2, 0):
            mine = at(q * WIDE + number(chip(order, AWAY[j], 0), core) * 8, 8, 8)
            first, second = (pl.ds((q * 8 + 2 * j + way) * 8, 8) for way in range(2))
            arrived(in_near.at[first, :], base + 10 + 2 * j)
            arrived(in_near.at[second, :], base + 10 + 2 * j + 1)
            lower_sum[mine, :] = lower_sum[mine, :] + (in_near[first, :] + in_near[second, :])
            if j == 3:
                for way, cols in enumerate((first_cols, second_cols)):
                    send(
                        total(q, chip(order, 2, 0), cols), in_cross_far.at[pl.ds((q * 2 + way) * 8, 8), :],
                        base + 18 + way, device(chip(order, 1 if way == 0 else 3, 0), core),
                    )

    def scatter_row(q):
        order, base = q % 2, (CHUNKS + q) * EXCHANGE
        for way, cols in enumerate((first_cols, second_cols)):
            step = 1 if way == 0 else 3
            to = chip(order, step, 0)
            came = pl.ds((q * 2 + way) * 8, 8)
            arrived(in_cross_far.at[came, :], base + 18 + way)
            mine = at(q * WIDE + number(to, core) * 8, 8, 8)
            lower_sum[mine, cols] = lower_sum[mine, cols] + in_cross_far[came, :]
            send(total(q, to), in_cross.at[came, :], base + 20 + way, device(to, core))

    def scatter_done(q):
        base = (CHUNKS + q) * EXCHANGE
        first, second = (pl.ds((q * 2 + way) * 8, 8) for way in range(2))
        arrived(in_cross.at[first, :], base + 20)
        arrived(in_cross.at[second, :], base + 21)
        mine = at(q * WIDE + me * 8, 8, 8)
        out[pl.ds(q * 8, 8), :] = lower_sum[mine, :] + (in_cross[first, :] + in_cross[second, :])

    def fetch(n, carry):
        rows = at(n * 256, 256, 256)
        pltpu.make_async_copy(upstream.at[rows, :], tile.at[rows, :], local_sem.at[n]).start()
        return carry

    lax.fori_loop(0, 8, fetch, 0)
    for q in range(CHUNKS):
        gathered[at(q * WIDE + me * 8, 8, 8), :] = panel[pl.ds(q * 8, 8), :]

    barrier = pltpu.get_barrier_semaphore()
    for first, second in ((1, 0), (3, 0), (0, 1), (0, 3)):
        pl.semaphore_signal(barrier, inc=1, device_id=device(chip(0, first, second), core), device_id_type=MESH)
    pl.semaphore_signal(barrier, inc=1, device_id=partner, device_id_type=MESH)
    for there, to in ((below, above_device), (child_up, up_device), (child_down, down_device)):
        @pl.when(there)
        def _():
            pl.semaphore_signal(barrier, inc=1, device_id=to, device_id_type=MESH)

    pl.semaphore_wait(barrier, 5 + sum(jnp.where(there, 1, 0) for there in (below, child_up, child_down)))

    def steps(pair):
        a, b = pair
        return [
            lambda: (gather_first(a), gather_first(b)),
            lambda: (gather_forward(a, 0), gather_forward(b, 0)),
            lambda: (gather_opposite(a), gather_opposite(b)),
            lambda: (gather_forward(a, 1), gather_forward(b, 1)),
            lambda: (gather_forward(a, 2), gather_forward(b, 2)),
            lambda: (gather_forward(a, 3), gather_forward(b, 3)),
            lambda: (gather_last(a), gather_last(b)),
            lambda: (gather_done(a), gather_done(b)),
        ]

    def begin(pair):
        for q in pair:
            gather_own_first(q)
        for q in pair:
            gather_own_second(q)

    begin((0, 1))
    prepare()
    early = steps((0, 1))
    for n, step in enumerate(early):
        if n == 5:
            begin((2, 3))
        step()
    z_start(0)
    z_start(1)

    plan = {}

    def add(n, task):
        plan.setdefault(n, []).append(task)

    add(0, lambda: upper(0))
    for n, step in enumerate(steps((2, 3))):
        add(n, step)
    add(2, lambda: upper(1))
    add(7, lambda: (z_start(2), z_start(3)))
    add(8, lambda: upper(2))
    add(9, lambda: upper(3))
    stages = (scatter_partner, scatter_far, scatter_near, scatter_column, scatter_row, scatter_done)
    for q in range(CHUNKS):
        add(12 + 4 * q, functools.partial(lower, q))
        for n, stage in enumerate(stages):
            add(14 + 4 * q + n, functools.partial(stage, q))
    rounds = PIECES + SKEW * DEPTH
    for n in range(max(plan) + 1):
        if n < rounds:
            z_round(n)
        for task in plan.get(n, ()):
            task()
        if n < rounds:
            sum_round(n)

    for one in sent:
        one.wait_send()

    def settle(k, carry):
        @pl.when(child_up)
        def _():
            z_copy(part(block, k), k, 0, up_device).wait_send()

        @pl.when(child_down)
        def _():
            z_copy(part(block, k), k, 1, down_device).wait_send()

        @pl.when(below)
        def _():
            sum_copy(k, 0).wait_send()

        return carry

    lax.fori_loop(0, PIECES, settle, 0)


def per_device(upstream, input_panel):
    f32, bf16 = jnp.float32, jnp.bfloat16
    total = CHUNKS * WIDE
    vmem = pltpu.VMEM
    result = pl.pallas_call(
        kernel,
        out_shape=jax.ShapeDtypeStruct((32, ROWS), f32),
        in_specs=[pl.BlockSpec(memory_space=pl.ANY), pl.BlockSpec(memory_space=pltpu.VMEM)],
        out_specs=pl.BlockSpec(memory_space=pltpu.VMEM),
        scratch_shapes=[
            vmem((total, ROWS), f32),
            vmem((total, COLS), f32),
            vmem((total, COLS), f32),
            vmem((2 * total, COLS), f32),
            vmem((total, ROWS), f32),
            vmem((total // 2, ROWS), f32),
            vmem((CHUNKS * 64, HALF), f32),
            vmem((CHUNKS * 64, ROWS), f32),
            vmem((CHUNKS * 16, HALF), f32),
            vmem((CHUNKS * 16, ROWS), f32),
            vmem((ROWS, COLS), f32),
            vmem((ROWS, COLS), bf16),
            vmem((ROWS, COLS), bf16),
            vmem((WIDE, ROWS), bf16),
            vmem((WIDE, ROWS), bf16),
            vmem((WIDE, COLS), bf16),
            vmem((WIDE, COLS), bf16),
            pltpu.SemaphoreType.DMA((2 * CHUNKS * EXCHANGE,)),
            pltpu.SemaphoreType.DMA((2 * CHUNKS * EXCHANGE,)),
            pltpu.SemaphoreType.DMA((3 * PIECES,)),
            pltpu.SemaphoreType.DMA((PIECES,)),
            pltpu.SemaphoreType.DMA((2 * PIECES,)),
            pltpu.SemaphoreType.DMA((8,)),
        ],
        compiler_params=pltpu.CompilerParams(
            collective_id=0, has_side_effects=True, vmem_limit_bytes=60 * 1024 * 1024
        ),
    )(upstream, input_panel.T)
    return result.T


def solution(mesh):
    placed = (P("row", ("col", "rep")), P("row", ("col", "rep")))
    return jax.shard_map(
        per_device, mesh=mesh, in_specs=placed, out_specs=P("row", ("col", "rep")), check_vma=False
    )
```

```python
import functools

import jax
import jax.numpy as jnp
from jax import lax
from jax.experimental import pallas as pl
from jax.experimental.pallas import tpu as pltpu
from jax.sharding import PartitionSpec as P

MESH = pl.DeviceIdType.MESH
ROWS = 2048
COLS = 512
HALF = ROWS // 2
CHUNKS = 4
WIDE = 256
PIECES = 32
PART = 32
PACK = 2
DEPTH = 5
SKEW = 3
AWAY = (0, 3, 1, 2)
STAGES = 20
LANES = 2 * CHUNKS * STAGES
COPIES = 2 * LANES + 6 * CHUNKS


def at(start, length, step):
    return pl.ds(pl.multiple_of(start, step), length)


def halves(x):
    high = x.astype(jnp.bfloat16)
    return high, (x - high.astype(jnp.float32)).astype(jnp.bfloat16)


def kernel(
    upstream, panel, out,
    gathered, block, upper_sum, upper_in, lower_sum,
    in_partner, in_far, in_near, in_cross_far, in_cross, in_root,
    tile, tile_high, tile_low, left_high, left_low, right_high, right_low,
    send_sem, recv_sem, z_send, z_down, z_up, root_send, root_recv, local_sem,
):
    row, col, rep = lax.axis_index("row"), lax.axis_index("col"), lax.axis_index("rep")
    core, x = lax.rem(col, 2), lax.div(rep, 2)
    y = lax.rem(rep, 2) * 2 + lax.div(col, 2)
    me = col * 8 + rep

    xs = [x] + [lax.rem(x + d, 4) for d in (1, 2, 3)]
    ys = [y] + [lax.rem(y + d, 4) for d in (1, 2, 3)]
    cols = [lax.rem(v, 2) * 2 for v in ys]
    reps = [[u * 2 + lax.div(v, 2) for v in ys] for u in xs]
    mine_at = [[((cols[b] + core) * 8 + reps[a][b]) * 8 for b in range(4)] for a in range(4)]

    def chip(order, first, second):
        return (first, second) if order == 0 else (second, first)

    def number(place):
        return mine_at[place[0]][place[1]]

    def device(place, on):
        return (row, cols[place[1]] + on, reps[place[0]][place[1]])

    low = lax.div(col, 2) * 4 + lax.div(x, 2)
    high = low + 2
    source = jnp.where(core == 0, low, high)
    offset = lax.rem(me, 4) * COLS
    active = row >= source
    root = row == source
    relay = (core == 0) & (low == 4) & (row == 2)
    below = (row > source) | relay
    member = active | relay
    upward = (core == 1) | (row <= high)
    child_up = ((core == 0) & (row >= low) & (row < high)) | ((core == 1) & (row >= high) & (row < 7))
    child_down = ((core == 0) & ((root & (high < 7)) | (row > high + 1))) | relay
    depth = jnp.where(relay, 1, jnp.where(upward, row - source, 8 - row + jnp.where(low == 4, 1, 0)))
    above = jnp.where(relay, 4, jnp.where(upward, row - 1, jnp.where(row < 7, row + 1, jnp.where(low == 4, 2, low))))
    up_device = (row + 1, col, rep)
    down_device = (jnp.where(root & (low == 4), 2, jnp.where(root | relay, 7, row - 1)), col, rep)
    above_device = (above, col, rep)
    slot = jnp.where(upward & jnp.logical_not(relay), 0, 1)

    def copy(src, dst, which, to):
        return pltpu.make_async_remote_copy(
            src_ref=src, dst_ref=dst, send_sem=send_sem.at[which], recv_sem=recv_sem.at[which],
            device_id=to, device_id_type=MESH,
        )

    sent = []

    def send(src, dst, which, to):
        one = copy(src, dst, which, to)
        one.start()
        sent.append(one)

    partner = (row, col + 1 - 2 * core, rep)

    def arrived(dst, which):
        copy(dst, dst, which, partner).wait_recv()

    def columns(h):
        return pl.ds(h * HALF, HALF)

    def quarter(h, way):
        return pl.ds(h * HALF + way * (HALF // 2), HALF // 2)

    def slab(q, place, cols):
        return gathered.at[at(q * WIDE + number(place), 8, 8), cols]

    def total(q, place, cols):
        return lower_sum.at[at(q * WIDE + number(place), 8, 8), cols]

    def group(ref, q, half, on):
        return ref.at[at(q * WIDE + half * 128 + on * 64, 64, 8), :]

    def gather_own(q):
        own = panel.at[pl.ds(q * 8, 8), :]
        for axis in range(2):
            for h in range(2):
                base, cols = (2 * q + h) * STAGES, columns(h)
                for way, step in enumerate((1, 3)):
                    to = chip(h, step, 0) if axis == 0 else chip(h, 0, step)
                    send(own.at[:, cols], slab(q, (0, 0), cols), base + (0 if axis == 0 else 4) + way, device(to, core))

    def gather_across(q, h, j):
        base = (2 * q + h) * STAGES + 4 + 2 * j
        piece = slab(q, chip(h, AWAY[j], 0), columns(h))
        send(piece, piece, base + 0, device(chip(h, 0, 1), core))
        send(piece, piece, base + 1, device(chip(h, 0, 3), core))

    def gather_first(q):
        for h in range(2):
            base = (2 * q + h) * STAGES
            arrived(slab(q, chip(h, 3, 0), columns(h)), base + 0)
            piece = slab(q, chip(h, 3, 0), quarter(h, 0))
            send(piece, piece, base + 2, device(chip(h, 1, 0), core))
            arrived(slab(q, chip(h, 1, 0), columns(h)), base + 1)
            piece = slab(q, chip(h, 1, 0), quarter(h, 1))
            send(piece, piece, base + 3, device(chip(h, 3, 0), core))
        for h in range(2):
            gather_across(q, h, 1)
            gather_across(q, h, 2)

    def gather_opposite(q):
        for h in range(2):
            base = (2 * q + h) * STAGES
            arrived(slab(q, chip(h, 2, 0), quarter(h, 0)), base + 2)
            arrived(slab(q, chip(h, 2, 0), quarter(h, 1)), base + 3)
            gather_across(q, h, 3)

    def gather_forward(q, j):
        for h in range(2):
            base = (2 * q + h) * STAGES + 4 + 2 * j
            arrived(slab(q, chip(h, AWAY[j], 3), columns(h)), base + 0)
            piece = slab(q, chip(h, AWAY[j], 3), quarter(h, 0))
            send(piece, piece, base + 8, device(chip(h, 0, 1), core))
            arrived(slab(q, chip(h, AWAY[j], 1), columns(h)), base + 1)
            piece = slab(q, chip(h, AWAY[j], 1), quarter(h, 1))
            send(piece, piece, base + 9, device(chip(h, 0, 3), core))

    def gather_last(q):
        for h in range(2):
            base = (2 * q + h) * STAGES + 12
            for j in range(4):
                arrived(slab(q, chip(h, AWAY[j], 2), quarter(h, 0)), base + 2 * j)
                arrived(slab(q, chip(h, AWAY[j], 2), quarter(h, 1)), base + 2 * j + 1)
        for half in range(2):
            piece = group(gathered, q, half, core)
            send(piece, piece, 2 * LANES + 2 * q + half, partner)

    def gather_done(q):
        for half in range(2):
            arrived(group(gathered, q, half, 1 - core), 2 * LANES + 2 * q + half)

    def part(ref, k, more=0):
        return ref.at[at(more + k * PART, PART, PART), :]

    def z_copy(src, k, way, to):
        return pltpu.make_async_remote_copy(
            src_ref=src, dst_ref=part(block, k), send_sem=z_send.at[way * PIECES + k], recv_sem=z_down.at[k],
            device_id=to, device_id_type=MESH,
        )

    def z_start(q):
        @pl.when(root)
        def _():
            def one(i, carry):
                k = q * (PIECES // CHUNKS) + i
                src = gathered.at[at(k * PART, PART, PART), at(offset, COLS, COLS)]

                @pl.when(child_up)
                def _():
                    z_copy(src, k, 0, up_device).start()

                @pl.when(child_down)
                def _():
                    z_copy(src, k, 1, down_device).start()

                return carry

            lax.fori_loop(0, PIECES // CHUNKS, one, 0)

    def z_round(step):
        first = (step - SKEW * (depth - 1)) * PACK

        @pl.when(below & (first >= 0) & (first < PIECES))
        def _():
            def one(i, carry):
                k = first + i
                src = part(block, k)
                z_copy(src, k, 0, up_device).wait_recv()

                @pl.when(child_up)
                def _():
                    z_copy(src, k, 0, up_device).start()

                @pl.when(child_down)
                def _():
                    z_copy(src, k, 1, down_device).start()

                return carry

            lax.fori_loop(0, PACK, one, 0)

    def sum_copy(k, which):
        return pltpu.make_async_remote_copy(
            src_ref=part(upper_sum, k), dst_ref=part(upper_in, k, which * PIECES * PART),
            send_sem=z_send.at[2 * PIECES + k], recv_sem=z_up.at[which * PIECES + k],
            device_id=above_device, device_id_type=MESH,
        )

    def owner_copy(k, i):
        c = lax.rem(k, WIDE // PART) * (PART // 8) + i
        q = lax.div(k, WIDE // PART)
        return c, q, pltpu.make_async_remote_copy(
            src_ref=upper_sum.at[at(k * PART + i * 8, 8, 8), :],
            dst_ref=in_root.at[at(q * 8, 8, 8), at(offset, COLS, COLS)],
            send_sem=root_send.at[k * (PART // 8) + i], recv_sem=root_recv.at[q * 4 + lax.rem(me, 4)],
            device_id=(row, lax.div(c, 8), lax.rem(c, 8)), device_id_type=MESH,
        )

    def to_owners(k):
        def one(i, carry):
            c, q, out_copy = owner_copy(k, i)

            @pl.when(c != me)
            def _():
                out_copy.start()

            @pl.when(c == me)
            def _():
                in_root[at(q * 8, 8, 8), at(offset, COLS, COLS)] = upper_sum[at(k * PART + i * 8, 8, 8), :]

            return carry

        lax.fori_loop(0, PART // 8, one, 0)

    def sum_round(step):
        first = (step - SKEW * (DEPTH - depth)) * PACK

        @pl.when(member & (first >= 0) & (first < PIECES))
        def _():
            def one(i, carry):
                k = first + i
                for which, there in enumerate((child_up, child_down)):
                    @pl.when(there)
                    def _():
                        sum_copy(k, which).wait_recv()
                        mine = at(k * PART, PART, PART)
                        other = at(which * PIECES * PART + k * PART, PART, PART)
                        upper_sum[mine, :] = upper_sum[mine, :] + upper_in[other, :]

                @pl.when(below)
                def _():
                    sum_copy(k, slot).start()

                @pl.when(root)
                def _():
                    to_owners(k)

                return carry

            lax.fori_loop(0, PACK, one, 0)

    def prepare():
        def one(n, carry):
            rows = at(n * 256, 256, 256)
            pltpu.make_async_copy(upstream.at[rows, :], tile.at[rows, :], local_sem.at[n]).wait()
            row_number = row * ROWS + n * 256 + lax.broadcasted_iota(jnp.int32, (256, COLS), 0)
            col_number = me * COLS + lax.broadcasted_iota(jnp.int32, (256, COLS), 1)
            kept = jnp.where(col_number <= row_number, tile[rows, :], 0.0)
            tile_high[rows, :], tile_low[rows, :] = halves(kept)
            return carry

        lax.fori_loop(0, 8, one, 0)

        @pl.when(relay)
        def _():
            def clear_relay(n, carry):
                upper_sum[at(n * 64, 64, 64), :] = jnp.zeros((64, COLS), jnp.float32)
                return carry

            lax.fori_loop(0, 16, clear_relay, 0)

        @pl.when(jnp.logical_not(active))
        def _():
            def clear(n, carry):
                lower_sum[at(n * 64, 64, 64), :] = jnp.zeros((64, ROWS), jnp.float32)
                return carry

            lax.fori_loop(0, 16, clear, 0)

    def product(left_a, left_b, right_a, right_b, dims):
        dot = functools.partial(
            lax.dot_general, dimension_numbers=(dims, ((), ())), preferred_element_type=jnp.float32
        )
        return dot(left_a, right_a) + dot(left_b, right_a) + dot(left_a, right_b)

    def upper(q, n):
        @pl.when(active)
        def _():
            here = pl.ds(q * WIDE, WIDE)

            def cut(i, carry):
                cols = at(i * 256, 256, 256)
                left_high[:, cols], left_low[:, cols] = halves(gathered[here, cols])
                return carry

            if n == 0:
                lax.fori_loop(0, 8, cut, 0)
            cols = pl.ds(n * 256, 256)
            upper_sum[here, cols] = product(
                left_high[...], left_low[...], tile_high[:, cols], tile_low[:, cols], ((1,), (0,))
            )

    def lower(q, n):
        @pl.when(active)
        def _():
            here = pl.ds(q * WIDE, WIDE)
            if n == 0:
                @pl.when(root)
                def _():
                    right_high[...], right_low[...] = halves(gathered[here, at(offset, COLS, COLS)])

                @pl.when(below)
                def _():
                    right_high[...], right_low[...] = halves(block[here, :])

            def one(i, carry):
                rows = at(n * HALF + i * 256, 256, 256)
                lower_sum[here, rows] = product(
                    right_high[...], right_low[...], tile_high[rows, :], tile_low[rows, :], ((1,), (1,))
                )
                return carry

            lax.fori_loop(0, 4, one, 0)

    def scatter_partner(q, h):
        for half in range(2):
            send(
                group(lower_sum, q, half, 1 - core).at[:, columns(h)],
                in_partner.at[pl.ds((q * 2 + half) * 64, 64), columns(h)],
                2 * LANES + 2 * CHUNKS + (2 * q + h) * 2 + half, partner,
            )

    def scatter_far(q, h):
        base = LANES + (2 * q + h) * STAGES
        for half in range(2):
            came = pl.ds((q * 2 + half) * 64, 64)
            arrived(in_partner.at[came, columns(h)], 2 * LANES + 2 * CHUNKS + (2 * q + h) * 2 + half)
            mine = at(q * WIDE + half * 128 + core * 64, 64, 8)
            lower_sum[mine, columns(h)] = lower_sum[mine, columns(h)] + in_partner[came, columns(h)]
        for j in (3, 1, 2, 0):
            for way, step in enumerate((1, 3)):
                send(
                    total(q, chip(h, AWAY[j], 2), quarter(h, way)),
                    in_far.at[pl.ds((q * 8 + 2 * j + way) * 8, 8), pl.ds(h * (HALF // 2), HALF // 2)],
                    base + 2 * j + way, device(chip(h, 0, step), core),
                )

    def scatter_near(q, h):
        base = LANES + (2 * q + h) * STAGES
        for j in (3, 1, 2, 0):
            for way, step in enumerate((1, 3)):
                to = chip(h, AWAY[j], step)
                came = pl.ds((q * 8 + 2 * j + way) * 8, 8)
                came_cols = pl.ds(h * (HALF // 2), HALF // 2)
                arrived(in_far.at[came, came_cols], base + 2 * j + way)
                mine, cols = at(q * WIDE + number(to), 8, 8), quarter(h, way)
                lower_sum[mine, cols] = lower_sum[mine, cols] + in_far[came, came_cols]
                send(
                    total(q, to, columns(h)), in_near.at[came, columns(h)], base + 8 + 2 * j + way,
                    device(chip(h, 0, step), core),
                )

    def scatter_column(q, h):
        base, cols = LANES + (2 * q + h) * STAGES, columns(h)
        for j in (3, 1, 2, 0):
            mine = at(q * WIDE + number(chip(h, AWAY[j], 0)), 8, 8)
            first, second = (pl.ds((q * 8 + 2 * j + way) * 8, 8) for way in range(2))
            arrived(in_near.at[first, cols], base + 8 + 2 * j)
            arrived(in_near.at[second, cols], base + 8 + 2 * j + 1)
            lower_sum[mine, cols] = lower_sum[mine, cols] + (in_near[first, cols] + in_near[second, cols])
            if j == 3:
                for way, step in enumerate((1, 3)):
                    send(
                        total(q, chip(h, 2, 0), quarter(h, way)),
                        in_cross_far.at[pl.ds((q * 2 + way) * 8, 8), pl.ds(h * (HALF // 2), HALF // 2)],
                        base + 16 + way, device(chip(h, step, 0), core),
                    )

    def scatter_row(q, h):
        base = LANES + (2 * q + h) * STAGES
        for way, step in enumerate((1, 3)):
            to = chip(h, step, 0)
            came = pl.ds((q * 2 + way) * 8, 8)
            came_cols = pl.ds(h * (HALF // 2), HALF // 2)
            arrived(in_cross_far.at[came, came_cols], base + 16 + way)
            mine, cols = at(q * WIDE + number(to), 8, 8), quarter(h, way)
            lower_sum[mine, cols] = lower_sum[mine, cols] + in_cross_far[came, came_cols]
            send(total(q, to, columns(h)), in_cross.at[came, columns(h)], base + 18 + way, device(to, core))

    def scatter_done(q, h):
        base, cols = LANES + (2 * q + h) * STAGES, columns(h)
        first, second = (pl.ds((q * 2 + way) * 8, 8) for way in range(2))
        arrived(in_cross.at[first, cols], base + 18)
        arrived(in_cross.at[second, cols], base + 19)
        mine = at(q * WIDE + me * 8, 8, 8)
        out[pl.ds(q * 8, 8), cols] = lower_sum[mine, cols] + (in_cross[first, cols] + in_cross[second, cols])

    def finish(q):
        here = pl.ds(q * 8, 8)
        for g in range(4):
            cols = pl.ds(g * COLS, COLS)

            @pl.when(me != row * 4 + g)
            def _():
                piece = in_root.at[here, cols]
                pltpu.make_async_remote_copy(
                    src_ref=piece, dst_ref=piece, send_sem=root_send.at[0], recv_sem=root_recv.at[q * 4 + g],
                    device_id=partner, device_id_type=MESH,
                ).wait_recv()

        out[here, :] = out[here, :] + in_root[here, :]

    def fetch(n, carry):
        rows = at(n * 256, 256, 256)
        pltpu.make_async_copy(upstream.at[rows, :], tile.at[rows, :], local_sem.at[n]).start()
        return carry

    lax.fori_loop(0, 8, fetch, 0)
    for q in range(CHUNKS):
        gathered[at(q * WIDE + me * 8, 8, 8), :] = panel[pl.ds(q * 8, 8), :]

    barrier = pltpu.get_barrier_semaphore()

    def greet(to):
        pl.semaphore_signal(barrier, inc=1, device_id=to, device_id_type=MESH)

    for first, second in ((1, 0), (3, 0), (0, 1), (0, 3)):
        greet(device(chip(0, first, second), core))
    greet(partner)
    for there, to in ((below, above_device), (child_up, up_device), (child_down, down_device)):
        @pl.when(there)
        def _():
            greet(to)

    for g in range(4):
        @pl.when(me != row * 4 + g)
        def _():
            c = row * 4 + g
            greet((row, lax.div(c, 8), lax.rem(c, 8)))

    pl.semaphore_wait(
        barrier, 5 + jnp.where(root, 31, 0) + sum(jnp.where(there, 1, 0) for there in (below, child_up, child_down))
    )

    plan = []

    def add(time, tag, task, *args):
        if tag in ON:
            plan.append((time, len(plan), functools.partial(task, *args)))

    schedule(add, locals())
    for _, _, task in sorted(plan, key=lambda entry: entry[:2]):
        task()

    for one in sent:
        one.wait_send()

    def settle(k, carry):
        if "z" in ON:
            @pl.when(child_up)
            def _():
                z_copy(part(block, k), k, 0, up_device).wait_send()

            @pl.when(child_down)
            def _():
                z_copy(part(block, k), k, 1, down_device).wait_send()

        if "r" in ON:
            @pl.when(below)
            def _():
                sum_copy(k, 0).wait_send()

            @pl.when(root)
            def _():
                for i in range(PART // 8):
                    c, _, out_copy = owner_copy(k, i)

                    @pl.when(c != me)
                    def _():
                        out_copy.wait_send()

        return carry

    lax.fori_loop(0, PIECES, settle, 0)


ON = "gpzruls"
GAP, LAST = 5.4, 0.0
GATHER = (0.0, 4.5, 6.0, 7.5, 9.0, 10.0, 12.0, 15.0, 17.5)
Z0, DZ, R0, DR = 21.0, 1.4, 30.0, 1.6
LOW0, LOWGAP = 43.0, 5.6
SCATTER = (1.3, 4.0, 7.0, 10.5, 13.5, 17.0)
FINISH = 200.0


def schedule(add, do):
    for q in range(CHUNKS):
        tasks = [
            (do["gather_own"], q), (do["gather_first"], q), (do["gather_forward"], q, 0), (do["gather_opposite"], q),
            (do["gather_forward"], q, 1), (do["gather_forward"], q, 2), (do["gather_forward"], q, 3),
            (do["gather_last"], q), (do["gather_done"], q),
        ]
        for time, task in zip(GATHER, tasks):
            add(GAP * q + time, "g", *task)
        done = GAP * q + GATHER[-1]
        add(done, "z", do["z_start"], q)
        for n in range(2):
            add(done + 0.1 + 1.3 * n, "u", do["upper"], q, n)
            low = LOW0 + LOWGAP * q + 1.8 * n
            add(low, "l", do["lower"], q, n)
            for time, stage in zip(SCATTER, ("partner", "far", "near", "column", "row", "done")):
                add(low + time, "s", do["scatter_" + stage], q, n)
        add(FINISH + q, "r", do["finish"], q)
    add(0.5, "p", do["prepare"])
    for n in range(PIECES // PACK + SKEW * (DEPTH - 1)):
        add(Z0 + DZ * n, "z", do["z_round"], n)
    for n in range(PIECES // PACK + SKEW * DEPTH):
        add(R0 + DR * n, "r", do["sum_round"], n)


def per_device(upstream, input_panel):
    f32, bf16 = jnp.float32, jnp.bfloat16
    total = CHUNKS * WIDE
    vmem = pltpu.VMEM
    result = pl.pallas_call(
        kernel,
        out_shape=jax.ShapeDtypeStruct((32, ROWS), f32),
        in_specs=[pl.BlockSpec(memory_space=pl.ANY), pl.BlockSpec(memory_space=pltpu.VMEM)],
        out_specs=pl.BlockSpec(memory_space=pltpu.VMEM),
        scratch_shapes=[
            vmem((total, ROWS), f32),
            vmem((total, COLS), f32),
            vmem((total, COLS), f32),
            vmem((2 * total, COLS), f32),
            vmem((total, ROWS), f32),
            vmem((total // 2, ROWS), f32),
            vmem((CHUNKS * 64, HALF), f32),
            vmem((CHUNKS * 64, ROWS), f32),
            vmem((CHUNKS * 16, HALF), f32),
            vmem((CHUNKS * 16, ROWS), f32),
            vmem((CHUNKS * 8, ROWS), f32),
            vmem((ROWS, COLS), f32),
            vmem((ROWS, COLS), bf16),
            vmem((ROWS, COLS), bf16),
            vmem((WIDE, ROWS), bf16),
            vmem((WIDE, ROWS), bf16),
            vmem((WIDE, COLS), bf16),
            vmem((WIDE, COLS), bf16),
            pltpu.SemaphoreType.DMA((COPIES,)),
            pltpu.SemaphoreType.DMA((COPIES,)),
            pltpu.SemaphoreType.DMA((3 * PIECES,)),
            pltpu.SemaphoreType.DMA((PIECES,)),
            pltpu.SemaphoreType.DMA((2 * PIECES,)),
            pltpu.SemaphoreType.DMA((PIECES * PART // 8,)),
            pltpu.SemaphoreType.DMA((CHUNKS * 4,)),
            pltpu.SemaphoreType.DMA((8,)),
        ],
        compiler_params=pltpu.CompilerParams(
            collective_id=0, has_side_effects=True, vmem_limit_bytes=60 * 1024 * 1024
        ),
    )(upstream, input_panel.T)
    return result.T


def solution(mesh):
    placed = (P("row", ("col", "rep")), P("row", ("col", "rep")))
    return jax.shard_map(
        per_device, mesh=mesh, in_specs=placed, out_specs=P("row", ("col", "rep")), check_vma=False
    )
```

```python
import functools

import jax
import jax.numpy as jnp
from jax import lax
from jax.experimental import pallas as pl
from jax.experimental.pallas import tpu as pltpu
from jax.sharding import PartitionSpec as P

MESH = pl.DeviceIdType.MESH
ROWS = 2048
COLS = 512
HALF = ROWS // 2
CHUNKS = 4
WIDE = 256
PIECES = 32
PART = 32
PACK = 1
DEPTH = 5
SKEW = 3
AWAY = (0, 3, 1, 2)
STAGES = 20
LANES = 2 * CHUNKS * STAGES
COPIES = 2 * LANES + 6 * CHUNKS


def at(start, length, step):
    return pl.ds(pl.multiple_of(start, step), length)


def halves(x):
    high = x.astype(jnp.bfloat16)
    return high, (x - high.astype(jnp.float32)).astype(jnp.bfloat16)


def kernel(
    upstream, panel, out,
    gathered, block, upper_sum, upper_in, lower_sum,
    in_partner, in_far, in_near, in_cross_far, in_cross, in_root,
    tile, tile_high, tile_low, left_high, left_low, right_high, right_low,
    send_sem, recv_sem, z_send, z_down, z_up, root_send, root_recv, local_sem,
):
    row, col, rep = lax.axis_index("row"), lax.axis_index("col"), lax.axis_index("rep")
    core, x = lax.rem(col, 2), lax.div(rep, 2)
    y = lax.rem(rep, 2) * 2 + lax.div(col, 2)
    me = col * 8 + rep

    xs = [x] + [lax.rem(x + d, 4) for d in (1, 2, 3)]
    ys = [y] + [lax.rem(y + d, 4) for d in (1, 2, 3)]
    cols = [lax.rem(v, 2) * 2 for v in ys]
    reps = [[u * 2 + lax.div(v, 2) for v in ys] for u in xs]
    mine_at = [[((cols[b] + core) * 8 + reps[a][b]) * 8 for b in range(4)] for a in range(4)]

    def chip(order, first, second):
        return (first, second) if order == 0 else (second, first)

    def number(place):
        return mine_at[place[0]][place[1]]

    def device(place, on):
        return (row, cols[place[1]] + on, reps[place[0]][place[1]])

    low = lax.div(col, 2) * 4 + lax.div(x, 2)
    high = low + 2
    source = jnp.where(core == 0, low, high)
    offset = lax.rem(me, 4) * COLS
    active = row >= source
    root = row == source
    relay = (core == 0) & (low == 4) & (row == 2)
    below = (row > source) | relay
    member = active | relay
    upward = (core == 1) | (row <= high)
    child_up = ((core == 0) & (row >= low) & (row < high)) | ((core == 1) & (row >= high) & (row < 7))
    child_down = ((core == 0) & ((root & (high < 7)) | (row > high + 1))) | relay
    depth = jnp.where(relay, 1, jnp.where(upward, row - source, 8 - row + jnp.where(low == 4, 1, 0)))
    above = jnp.where(relay, 4, jnp.where(upward, row - 1, jnp.where(row < 7, row + 1, jnp.where(low == 4, 2, low))))
    up_device = (row + 1, col, rep)
    down_device = (jnp.where(root & (low == 4), 2, jnp.where(root | relay, 7, row - 1)), col, rep)
    above_device = (above, col, rep)
    slot = jnp.where(upward & jnp.logical_not(relay), 0, 1)

    def copy(src, dst, which, to):
        return pltpu.make_async_remote_copy(
            src_ref=src, dst_ref=dst, send_sem=send_sem.at[which], recv_sem=recv_sem.at[which],
            device_id=to, device_id_type=MESH,
        )

    sent = []

    def send(src, dst, which, to):
        one = copy(src, dst, which, to)
        one.start()
        sent.append(one)

    partner = (row, col + 1 - 2 * core, rep)

    def arrived(dst, which):
        copy(dst, dst, which, partner).wait_recv()

    def columns(h):
        return pl.ds(h * HALF, HALF)

    def quarter(h, way):
        return pl.ds(h * HALF + way * (HALF // 2), HALF // 2)

    def slab(q, place, cols):
        return gathered.at[at(q * WIDE + number(place), 8, 8), cols]

    def total(q, place, cols):
        return lower_sum.at[at(q * WIDE + number(place), 8, 8), cols]

    def group(ref, q, half, on):
        return ref.at[at(q * WIDE + half * 128 + on * 64, 64, 8), :]

    def gather_own(q):
        own = panel.at[pl.ds(q * 8, 8), :]
        for axis in range(2):
            for h in range(2):
                base, cols = (2 * q + h) * STAGES, columns(h)
                for way, step in enumerate((1, 3)):
                    to = chip(h, step, 0) if axis == 0 else chip(h, 0, step)
                    send(own.at[:, cols], slab(q, (0, 0), cols), base + (0 if axis == 0 else 4) + way, device(to, core))

    def gather_across(q, h, j):
        base = (2 * q + h) * STAGES + 4 + 2 * j
        piece = slab(q, chip(h, AWAY[j], 0), columns(h))
        send(piece, piece, base + 0, device(chip(h, 0, 1), core))
        send(piece, piece, base + 1, device(chip(h, 0, 3), core))

    def gather_first(q):
        for h in range(2):
            base = (2 * q + h) * STAGES
            arrived(slab(q, chip(h, 3, 0), columns(h)), base + 0)
            piece = slab(q, chip(h, 3, 0), quarter(h, 0))
            send(piece, piece, base + 2, device(chip(h, 1, 0), core))
            arrived(slab(q, chip(h, 1, 0), columns(h)), base + 1)
            piece = slab(q, chip(h, 1, 0), quarter(h, 1))
            send(piece, piece, base + 3, device(chip(h, 3, 0), core))
        for h in range(2):
            gather_across(q, h, 1)
            gather_across(q, h, 2)

    def gather_opposite(q):
        for h in range(2):
            base = (2 * q + h) * STAGES
            arrived(slab(q, chip(h, 2, 0), quarter(h, 0)), base + 2)
            arrived(slab(q, chip(h, 2, 0), quarter(h, 1)), base + 3)
            gather_across(q, h, 3)

    def gather_forward(q, j):
        for h in range(2):
            base = (2 * q + h) * STAGES + 4 + 2 * j
            arrived(slab(q, chip(h, AWAY[j], 3), columns(h)), base + 0)
            piece = slab(q, chip(h, AWAY[j], 3), quarter(h, 0))
            send(piece, piece, base + 8, device(chip(h, 0, 1), core))
            arrived(slab(q, chip(h, AWAY[j], 1), columns(h)), base + 1)
            piece = slab(q, chip(h, AWAY[j], 1), quarter(h, 1))
            send(piece, piece, base + 9, device(chip(h, 0, 3), core))

    def gather_last(q):
        for h in range(2):
            base = (2 * q + h) * STAGES + 12
            for j in range(4):
                arrived(slab(q, chip(h, AWAY[j], 2), quarter(h, 0)), base + 2 * j)
                arrived(slab(q, chip(h, AWAY[j], 2), quarter(h, 1)), base + 2 * j + 1)
        for half in range(2):
            piece = group(gathered, q, half, core)
            send(piece, piece, 2 * LANES + 2 * q + half, partner)

    def gather_done(q):
        for half in range(2):
            arrived(group(gathered, q, half, 1 - core), 2 * LANES + 2 * q + half)

    def part(ref, k, more=0):
        return ref.at[at(more + k * PART, PART, PART), :]

    def z_copy(src, k, way, to):
        return pltpu.make_async_remote_copy(
            src_ref=src, dst_ref=part(block, k), send_sem=z_send.at[way * PIECES + k], recv_sem=z_down.at[k],
            device_id=to, device_id_type=MESH,
        )

    def z_start(q):
        @pl.when(root)
        def _():
            def one(i, carry):
                k = q * (PIECES // CHUNKS) + i
                src = gathered.at[at(k * PART, PART, PART), at(offset, COLS, COLS)]

                @pl.when(child_up)
                def _():
                    z_copy(src, k, 0, up_device).start()

                @pl.when(child_down)
                def _():
                    z_copy(src, k, 1, down_device).start()

                return carry

            lax.fori_loop(0, PIECES // CHUNKS, one, 0)

    def z_round(step):
        first = (step - SKEW * (depth - 1)) * PACK

        @pl.when(below & (first >= 0) & (first < PIECES))
        def _():
            def one(i, carry):
                k = first + i
                src = part(block, k)
                z_copy(src, k, 0, up_device).wait_recv()

                @pl.when(child_up)
                def _():
                    z_copy(src, k, 0, up_device).start()

                @pl.when(child_down)
                def _():
                    z_copy(src, k, 1, down_device).start()

                return carry

            lax.fori_loop(0, PACK, one, 0)

    def sum_copy(k, which):
        return pltpu.make_async_remote_copy(
            src_ref=part(upper_sum, k), dst_ref=part(upper_in, k, which * PIECES * PART),
            send_sem=z_send.at[2 * PIECES + k], recv_sem=z_up.at[which * PIECES + k],
            device_id=above_device, device_id_type=MESH,
        )

    def owner_copy(k, i):
        c = lax.rem(k, WIDE // PART) * (PART // 8) + i
        q = lax.div(k, WIDE // PART)
        return c, q, pltpu.make_async_remote_copy(
            src_ref=upper_sum.at[at(k * PART + i * 8, 8, 8), :],
            dst_ref=in_root.at[at(q * 8, 8, 8), at(offset, COLS, COLS)],
            send_sem=root_send.at[k * (PART // 8) + i], recv_sem=root_recv.at[q * 4 + lax.rem(me, 4)],
            device_id=(row, lax.div(c, 8), lax.rem(c, 8)), device_id_type=MESH,
        )

    def to_owners(k):
        def one(i, carry):
            c, q, out_copy = owner_copy(k, i)

            @pl.when(c != me)
            def _():
                out_copy.start()

            @pl.when(c == me)
            def _():
                in_root[at(q * 8, 8, 8), at(offset, COLS, COLS)] = upper_sum[at(k * PART + i * 8, 8, 8), :]

            return carry

        lax.fori_loop(0, PART // 8, one, 0)

    def sum_round(step):
        first = (step - SKEW * (DEPTH - depth)) * PACK

        @pl.when(member & (first >= 0) & (first < PIECES))
        def _():
            def one(i, carry):
                k = first + i
                for which, there in enumerate((child_up, child_down)):
                    @pl.when(there)
                    def _():
                        sum_copy(k, which).wait_recv()
                        mine = at(k * PART, PART, PART)
                        other = at(which * PIECES * PART + k * PART, PART, PART)
                        upper_sum[mine, :] = upper_sum[mine, :] + upper_in[other, :]

                @pl.when(below)
                def _():
                    sum_copy(k, slot).start()

                @pl.when(root)
                def _():
                    to_owners(k)

                return carry

            lax.fori_loop(0, PACK, one, 0)

    def prepare():
        def one(n, carry):
            rows = at(n * 256, 256, 256)
            pltpu.make_async_copy(upstream.at[rows, :], tile.at[rows, :], local_sem.at[n]).wait()
            row_number = row * ROWS + n * 256 + lax.broadcasted_iota(jnp.int32, (256, COLS), 0)
            col_number = me * COLS + lax.broadcasted_iota(jnp.int32, (256, COLS), 1)
            kept = jnp.where(col_number <= row_number, tile[rows, :], 0.0)
            tile_high[rows, :], tile_low[rows, :] = halves(kept)
            return carry

        lax.fori_loop(0, 8, one, 0)

        @pl.when(relay)
        def _():
            def clear_relay(n, carry):
                upper_sum[at(n * 64, 64, 64), :] = jnp.zeros((64, COLS), jnp.float32)
                return carry

            lax.fori_loop(0, 16, clear_relay, 0)

        @pl.when(jnp.logical_not(active))
        def _():
            def clear(n, carry):
                lower_sum[at(n * 64, 64, 64), :] = jnp.zeros((64, ROWS), jnp.float32)
                return carry

            lax.fori_loop(0, 16, clear, 0)

    def product(left_a, left_b, right_a, right_b, dims):
        dot = functools.partial(
            lax.dot_general, dimension_numbers=(dims, ((), ())), preferred_element_type=jnp.float32
        )
        return dot(left_a, right_a) + dot(left_b, right_a) + dot(left_a, right_b)

    def upper(q, n):
        @pl.when(active)
        def _():
            here = pl.ds(q * WIDE, WIDE)

            def cut(i, carry):
                cols = at(i * 256, 256, 256)
                left_high[:, cols], left_low[:, cols] = halves(gathered[here, cols])
                return carry

            if n == 0:
                lax.fori_loop(0, 8, cut, 0)
            cols = pl.ds(n * 256, 256)
            upper_sum[here, cols] = product(
                left_high[...], left_low[...], tile_high[:, cols], tile_low[:, cols], ((1,), (0,))
            )

    def lower(q, n):
        @pl.when(active)
        def _():
            here = pl.ds(q * WIDE, WIDE)
            if n == 0:
                @pl.when(root)
                def _():
                    right_high[...], right_low[...] = halves(gathered[here, at(offset, COLS, COLS)])

                @pl.when(below)
                def _():
                    right_high[...], right_low[...] = halves(block[here, :])

            def one(i, carry):
                rows = at(n * HALF + i * 256, 256, 256)
                lower_sum[here, rows] = product(
                    right_high[...], right_low[...], tile_high[rows, :], tile_low[rows, :], ((1,), (1,))
                )
                return carry

            lax.fori_loop(0, 4, one, 0)

    def scatter_partner(q, h):
        for half in range(2):
            send(
                group(lower_sum, q, half, 1 - core).at[:, columns(h)],
                in_partner.at[pl.ds((q * 2 + half) * 64, 64), columns(h)],
                2 * LANES + 2 * CHUNKS + (2 * q + h) * 2 + half, partner,
            )

    def scatter_far(q, h):
        base = LANES + (2 * q + h) * STAGES
        for half in range(2):
            came = pl.ds((q * 2 + half) * 64, 64)
            arrived(in_partner.at[came, columns(h)], 2 * LANES + 2 * CHUNKS + (2 * q + h) * 2 + half)
            mine = at(q * WIDE + half * 128 + core * 64, 64, 8)
            lower_sum[mine, columns(h)] = lower_sum[mine, columns(h)] + in_partner[came, columns(h)]
        for j in (3, 1, 2, 0):
            for way, step in enumerate((1, 3)):
                send(
                    total(q, chip(h, AWAY[j], 2), quarter(h, way)),
                    in_far.at[pl.ds((q * 8 + 2 * j + way) * 8, 8), pl.ds(h * (HALF // 2), HALF // 2)],
                    base + 2 * j + way, device(chip(h, 0, step), core),
                )

    def scatter_near(q, h):
        base = LANES + (2 * q + h) * STAGES
        for j in (3, 1, 2, 0):
            for way, step in enumerate((1, 3)):
                to = chip(h, AWAY[j], step)
                came = pl.ds((q * 8 + 2 * j + way) * 8, 8)
                came_cols = pl.ds(h * (HALF // 2), HALF // 2)
                arrived(in_far.at[came, came_cols], base + 2 * j + way)
                mine, cols = at(q * WIDE + number(to), 8, 8), quarter(h, way)
                lower_sum[mine, cols] = lower_sum[mine, cols] + in_far[came, came_cols]
                send(
                    total(q, to, columns(h)), in_near.at[came, columns(h)], base + 8 + 2 * j + way,
                    device(chip(h, 0, step), core),
                )

    def scatter_column(q, h):
        base, cols = LANES + (2 * q + h) * STAGES, columns(h)
        for j in (3, 1, 2, 0):
            mine = at(q * WIDE + number(chip(h, AWAY[j], 0)), 8, 8)
            first, second = (pl.ds((q * 8 + 2 * j + way) * 8, 8) for way in range(2))
            arrived(in_near.at[first, cols], base + 8 + 2 * j)
            arrived(in_near.at[second, cols], base + 8 + 2 * j + 1)
            lower_sum[mine, cols] = lower_sum[mine, cols] + (in_near[first, cols] + in_near[second, cols])
            if j == 3:
                for way, step in enumerate((1, 3)):
                    send(
                        total(q, chip(h, 2, 0), quarter(h, way)),
                        in_cross_far.at[pl.ds((q * 2 + way) * 8, 8), pl.ds(h * (HALF // 2), HALF // 2)],
                        base + 16 + way, device(chip(h, step, 0), core),
                    )

    def scatter_row(q, h):
        base = LANES + (2 * q + h) * STAGES
        for way, step in enumerate((1, 3)):
            to = chip(h, step, 0)
            came = pl.ds((q * 2 + way) * 8, 8)
            came_cols = pl.ds(h * (HALF // 2), HALF // 2)
            arrived(in_cross_far.at[came, came_cols], base + 16 + way)
            mine, cols = at(q * WIDE + number(to), 8, 8), quarter(h, way)
            lower_sum[mine, cols] = lower_sum[mine, cols] + in_cross_far[came, came_cols]
            send(total(q, to, columns(h)), in_cross.at[came, columns(h)], base + 18 + way, device(to, core))

    def scatter_done(q, h):
        base, cols = LANES + (2 * q + h) * STAGES, columns(h)
        first, second = (pl.ds((q * 2 + way) * 8, 8) for way in range(2))
        arrived(in_cross.at[first, cols], base + 18)
        arrived(in_cross.at[second, cols], base + 19)
        mine = at(q * WIDE + me * 8, 8, 8)
        out[pl.ds(q * 8, 8), cols] = lower_sum[mine, cols] + (in_cross[first, cols] + in_cross[second, cols])

    def finish(q):
        here = pl.ds(q * 8, 8)
        for g in range(4):
            cols = pl.ds(g * COLS, COLS)

            @pl.when(me != row * 4 + g)
            def _():
                piece = in_root.at[here, cols]
                pltpu.make_async_remote_copy(
                    src_ref=piece, dst_ref=piece, send_sem=root_send.at[0], recv_sem=root_recv.at[q * 4 + g],
                    device_id=partner, device_id_type=MESH,
                ).wait_recv()

        out[here, :] = out[here, :] + in_root[here, :]

    def fetch(n, carry):
        rows = at(n * 256, 256, 256)
        pltpu.make_async_copy(upstream.at[rows, :], tile.at[rows, :], local_sem.at[n]).start()
        return carry

    lax.fori_loop(0, 8, fetch, 0)
    for q in range(CHUNKS):
        gathered[at(q * WIDE + me * 8, 8, 8), :] = panel[pl.ds(q * 8, 8), :]

    barrier = pltpu.get_barrier_semaphore()

    def greet(to):
        pl.semaphore_signal(barrier, inc=1, device_id=to, device_id_type=MESH)

    for first, second in ((1, 0), (3, 0), (0, 1), (0, 3)):
        greet(device(chip(0, first, second), core))
    greet(partner)
    for there, to in ((below, above_device), (child_up, up_device), (child_down, down_device)):
        @pl.when(there)
        def _():
            greet(to)

    for g in range(4):
        @pl.when(me != row * 4 + g)
        def _():
            c = row * 4 + g
            greet((row, lax.div(c, 8), lax.rem(c, 8)))

    pl.semaphore_wait(
        barrier, 5 + jnp.where(root, 31, 0) + sum(jnp.where(there, 1, 0) for there in (below, child_up, child_down))
    )

    tasks = locals()
    for which, *args in ORDER:
        tasks[TASKS[which]](*args)

    for one in sent:
        one.wait_send()

    def settle(k, carry):
        if True:
            @pl.when(child_up)
            def _():
                z_copy(part(block, k), k, 0, up_device).wait_send()

            @pl.when(child_down)
            def _():
                z_copy(part(block, k), k, 1, down_device).wait_send()

        if True:
            @pl.when(below)
            def _():
                sum_copy(k, 0).wait_send()

            @pl.when(root)
            def _():
                for i in range(PART // 8):
                    c, _, out_copy = owner_copy(k, i)

                    @pl.when(c != me)
                    def _():
                        out_copy.wait_send()

        return carry

    lax.fori_loop(0, PIECES, settle, 0)


TASKS = (
    "gather_own",
    "prepare",
    "gather_first",
    "gather_opposite",
    "gather_forward",
    "gather_last",
    "gather_done",
    "z_start",
    "upper",
    "z_round",
    "sum_round",
    "lower",
    "scatter_partner",
    "scatter_far",
    "scatter_near",
    "scatter_column",
    "scatter_row",
    "scatter_done",
    "finish",
)
ORDER = (
    (0, 0), (1,), (2, 0), (0, 1), (3, 0), (4, 0, 0), (4, 0, 1), (2, 1), (4, 0, 2), (4, 0, 3), (4, 1, 0),
    (3, 1), (0, 2), (4, 1, 2), (5, 0), (2, 2), (6, 0), (7, 0), (4, 1, 3), (4, 1, 1), (0, 3), (8, 0, 0),
    (9, 0), (8, 0, 1), (9, 1), (3, 2), (4, 2, 0), (5, 1), (9, 2), (2, 3), (4, 2, 2), (9, 3), (9, 4), (9, 5),
    (10, 0), (6, 1), (4, 2, 3), (7, 1), (10, 1), (10, 2), (4, 2, 1), (9, 6), (8, 1, 0), (10, 3), (10, 4),
    (9, 7), (9, 8), (5, 2), (4, 3, 0), (3, 3), (10, 5), (9, 9), (8, 1, 1), (10, 6), (9, 10), (10, 7), (6, 2),
    (9, 11), (4, 3, 1), (7, 2), (10, 8), (8, 2, 0), (10, 9), (9, 12), (9, 13), (10, 10), (4, 3, 2), (4, 3, 3),
    (9, 14), (8, 2, 1), (9, 15), (10, 11), (9, 16), (5, 3), (9, 17), (10, 12), (9, 18), (10, 13), (9, 19),
    (6, 3), (9, 20), (10, 14), (8, 3, 0), (9, 21), (7, 3), (10, 15), (9, 22), (11, 0, 0), (12, 0, 0),
    (10, 16), (9, 23), (11, 0, 1), (12, 0, 1), (9, 24), (9, 25), (10, 17), (9, 26), (10, 18), (13, 0, 0),
    (8, 3, 1), (9, 27), (10, 19), (13, 0, 1), (9, 28), (11, 1, 0), (9, 29), (10, 20), (10, 21), (12, 1, 0),
    (9, 30), (11, 1, 1), (9, 31), (10, 22), (14, 0, 0), (12, 1, 1), (10, 23), (9, 32), (10, 24), (14, 0, 1),
    (13, 1, 0), (9, 33), (10, 25), (13, 1, 1), (15, 0, 0), (9, 34), (10, 26), (9, 35), (11, 2, 0), (10, 27),
    (10, 28), (9, 36), (9, 37), (15, 0, 1), (14, 1, 0), (10, 29), (12, 2, 0), (14, 1, 1), (11, 2, 1), (9, 38),
    (12, 2, 1), (10, 30), (9, 39), (10, 31), (13, 2, 1), (13, 2, 0), (9, 40), (10, 32), (16, 0, 1), (9, 41),
    (15, 1, 0), (10, 33), (16, 0, 0), (15, 1, 1), (9, 42), (10, 34), (9, 43), (11, 3, 0), (10, 35),
    (14, 2, 0), (12, 3, 0), (14, 2, 1), (11, 3, 1), (17, 0, 0), (12, 3, 1), (10, 36), (10, 37), (10, 38),
    (13, 3, 0), (13, 3, 1), (16, 1, 0), (10, 39), (15, 2, 1), (10, 40), (15, 2, 0), (10, 41), (14, 3, 0),
    (14, 3, 1), (10, 42), (16, 2, 1), (16, 1, 1), (10, 43), (16, 2, 0), (15, 3, 0), (15, 3, 1), (10, 44),
    (10, 45), (17, 0, 1), (10, 46), (18, 0), (16, 3, 0), (17, 2, 0), (17, 1, 0), (16, 3, 1), (17, 3, 0),
    (17, 2, 1), (17, 1, 1), (18, 2), (18, 1), (17, 3, 1), (18, 3),
)


def per_device(upstream, input_panel):
    f32, bf16 = jnp.float32, jnp.bfloat16
    total = CHUNKS * WIDE
    vmem = pltpu.VMEM
    result = pl.pallas_call(
        kernel,
        out_shape=jax.ShapeDtypeStruct((32, ROWS), f32),
        in_specs=[pl.BlockSpec(memory_space=pl.ANY), pl.BlockSpec(memory_space=pltpu.VMEM)],
        out_specs=pl.BlockSpec(memory_space=pltpu.VMEM),
        scratch_shapes=[
            vmem((total, ROWS), f32),
            vmem((total, COLS), f32),
            vmem((total, COLS), f32),
            vmem((2 * total, COLS), f32),
            vmem((total, ROWS), f32),
            vmem((total // 2, ROWS), f32),
            vmem((CHUNKS * 64, HALF), f32),
            vmem((CHUNKS * 64, ROWS), f32),
            vmem((CHUNKS * 16, HALF), f32),
            vmem((CHUNKS * 16, ROWS), f32),
            vmem((CHUNKS * 8, ROWS), f32),
            vmem((ROWS, COLS), f32),
            vmem((ROWS, COLS), bf16),
            vmem((ROWS, COLS), bf16),
            vmem((WIDE, ROWS), bf16),
            vmem((WIDE, ROWS), bf16),
            vmem((WIDE, COLS), bf16),
            vmem((WIDE, COLS), bf16),
            pltpu.SemaphoreType.DMA((COPIES,)),
            pltpu.SemaphoreType.DMA((COPIES,)),
            pltpu.SemaphoreType.DMA((3 * PIECES,)),
            pltpu.SemaphoreType.DMA((PIECES,)),
            pltpu.SemaphoreType.DMA((2 * PIECES,)),
            pltpu.SemaphoreType.DMA((PIECES * PART // 8,)),
            pltpu.SemaphoreType.DMA((CHUNKS * 4,)),
            pltpu.SemaphoreType.DMA((8,)),
        ],
        compiler_params=pltpu.CompilerParams(
            collective_id=0, has_side_effects=True, vmem_limit_bytes=60 * 1024 * 1024
        ),
    )(upstream, input_panel.T)
    return result.T


def solution(mesh):
    placed = (P("row", ("col", "rep")), P("row", ("col", "rep")))
    return jax.shard_map(
        per_device, mesh=mesh, in_specs=placed, out_specs=P("row", ("col", "rep")), check_vma=False
    )
```

```python
import functools

import jax
import jax.numpy as jnp
from jax import lax
from jax.experimental import pallas as pl
from jax.experimental.pallas import tpu as pltpu
from jax.sharding import PartitionSpec as P

MESH = pl.DeviceIdType.MESH
ROWS = 2048
COLS = 512
HALF = ROWS // 2
CHUNKS = 4
WIDE = 256
PIECES = 32
PART = 32
PACK = 1
DEPTH = 5
SKEW = 3
AWAY = (0, 3, 1, 2)
STAGES = 20
LANES = 2 * CHUNKS * STAGES
COPIES = 2 * LANES + 6 * CHUNKS


def at(start, length, step):
    return pl.ds(pl.multiple_of(start, step), length)


def halves(x):
    high = x.astype(jnp.bfloat16)
    return high, (x - high.astype(jnp.float32)).astype(jnp.bfloat16)


def kernel(
    upstream, panel, out,
    gathered, block, upper_sum, side_sum, upper_in, lower_sum,
    in_partner, in_far, in_near, in_cross_far, in_cross, in_root,
    tile, tile_high, tile_low, left_high, left_low, right_high, right_low,
    send_sem, recv_sem, z_send, z_down, z_up, root_send, root_recv, side_send, side_recv, local_sem,
):
    row, col, rep = lax.axis_index("row"), lax.axis_index("col"), lax.axis_index("rep")
    core, x = lax.rem(col, 2), lax.div(rep, 2)
    y = lax.rem(rep, 2) * 2 + lax.div(col, 2)
    me = col * 8 + rep

    xs = [x] + [lax.rem(x + d, 4) for d in (1, 2, 3)]
    ys = [y] + [lax.rem(y + d, 4) for d in (1, 2, 3)]
    cols = [lax.rem(v, 2) * 2 for v in ys]
    reps = [[u * 2 + lax.div(v, 2) for v in ys] for u in xs]
    mine_at = [[((cols[b] + core) * 8 + reps[a][b]) * 8 for b in range(4)] for a in range(4)]

    def chip(order, first, second):
        return (first, second) if order == 0 else (second, first)

    def number(place):
        return mine_at[place[0]][place[1]]

    def device(place, on):
        return (row, cols[place[1]] + on, reps[place[0]][place[1]])

    low = lax.div(col, 2) * 4 + lax.div(x, 2)
    high = low + 2
    offset = lax.rem(me, 4) * COLS

    def line(first):
        second = jnp.logical_not(first)
        source = jnp.where(first, low, high)
        relay = first & (low == 4) & (row == 2)
        root, active = row == source, row >= source
        upward = second | (row <= high)
        child_up = (first & (row >= low) & (row < high)) | (second & (row >= high) & (row < 7))
        child_down = (first & ((root & (high < 7)) | (row > high + 1))) | relay
        depth = jnp.where(relay, 1, jnp.where(upward, row - source, 8 - row + jnp.where(low == 4, 1, 0)))
        far = jnp.where(row < 7, row + 1, jnp.where(low == 4, 2, low))
        above = jnp.where(relay, 4, jnp.where(upward, row - 1, far))
        down = jnp.where(root & (low == 4), 2, jnp.where(root | relay, 7, row - 1))
        slot = jnp.where(upward & jnp.logical_not(relay), 0, 1)
        return root, active, relay, active & jnp.logical_not(root) | relay, child_up, child_down, depth, above, down, slot

    root, active, _, below, child_up, child_down, depth, above, down, _ = line(core == 0)
    sum_root, sum_active, sum_relay, sum_below, sum_up, sum_down, sum_depth, sum_above, sum_below_row, sum_slot = line(core == 1)
    up_device = (row + 1, col, rep)
    down_device = (down, col, rep)
    above_device = (above, col, rep)

    def copy(src, dst, which, to):
        return pltpu.make_async_remote_copy(
            src_ref=src, dst_ref=dst, send_sem=send_sem.at[which], recv_sem=recv_sem.at[which],
            device_id=to, device_id_type=MESH,
        )

    sent = []

    def send(src, dst, which, to):
        one = copy(src, dst, which, to)
        one.start()
        sent.append(one)

    partner = (row, col + 1 - 2 * core, rep)

    def arrived(dst, which):
        copy(dst, dst, which, partner).wait_recv()

    def columns(h):
        return pl.ds(h * HALF, HALF)

    def quarter(h, way):
        return pl.ds(h * HALF + way * (HALF // 2), HALF // 2)

    def slab(q, place, cols):
        return gathered.at[at(q * WIDE + number(place), 8, 8), cols]

    def total(q, place, cols):
        return lower_sum.at[at(q * WIDE + number(place), 8, 8), cols]

    def group(ref, q, half, on):
        return ref.at[at(q * WIDE + half * 128 + on * 64, 64, 8), :]

    def gather_own(q):
        own = panel.at[pl.ds(q * 8, 8), :]
        for axis in range(2):
            for h in range(2):
                base, cols = (2 * q + h) * STAGES, columns(h)
                for way, step in enumerate((1, 3)):
                    to = chip(h, step, 0) if axis == 0 else chip(h, 0, step)
                    send(own.at[:, cols], slab(q, (0, 0), cols), base + (0 if axis == 0 else 4) + way, device(to, core))

    def gather_across(q, h, j):
        base = (2 * q + h) * STAGES + 4 + 2 * j
        piece = slab(q, chip(h, AWAY[j], 0), columns(h))
        send(piece, piece, base + 0, device(chip(h, 0, 1), core))
        send(piece, piece, base + 1, device(chip(h, 0, 3), core))

    def gather_first(q):
        for h in range(2):
            base = (2 * q + h) * STAGES
            arrived(slab(q, chip(h, 3, 0), columns(h)), base + 0)
            piece = slab(q, chip(h, 3, 0), quarter(h, 0))
            send(piece, piece, base + 2, device(chip(h, 1, 0), core))
            arrived(slab(q, chip(h, 1, 0), columns(h)), base + 1)
            piece = slab(q, chip(h, 1, 0), quarter(h, 1))
            send(piece, piece, base + 3, device(chip(h, 3, 0), core))
        for h in range(2):
            gather_across(q, h, 1)
            gather_across(q, h, 2)

    def gather_opposite(q):
        for h in range(2):
            base = (2 * q + h) * STAGES
            arrived(slab(q, chip(h, 2, 0), quarter(h, 0)), base + 2)
            arrived(slab(q, chip(h, 2, 0), quarter(h, 1)), base + 3)
            gather_across(q, h, 3)

    def gather_forward(q, j):
        for h in range(2):
            base = (2 * q + h) * STAGES + 4 + 2 * j
            arrived(slab(q, chip(h, AWAY[j], 3), columns(h)), base + 0)
            piece = slab(q, chip(h, AWAY[j], 3), quarter(h, 0))
            send(piece, piece, base + 8, device(chip(h, 0, 1), core))
            arrived(slab(q, chip(h, AWAY[j], 1), columns(h)), base + 1)
            piece = slab(q, chip(h, AWAY[j], 1), quarter(h, 1))
            send(piece, piece, base + 9, device(chip(h, 0, 3), core))

    def gather_last(q):
        for h in range(2):
            base = (2 * q + h) * STAGES + 12
            for j in range(4):
                arrived(slab(q, chip(h, AWAY[j], 2), quarter(h, 0)), base + 2 * j)
                arrived(slab(q, chip(h, AWAY[j], 2), quarter(h, 1)), base + 2 * j + 1)
        for half in range(2):
            piece = group(gathered, q, half, core)
            send(piece, piece, 2 * LANES + 2 * q + half, partner)

    def gather_done(q):
        for half in range(2):
            arrived(group(gathered, q, half, 1 - core), 2 * LANES + 2 * q + half)

    def part(ref, k, more=0):
        return ref.at[at(more + k * PART, PART, PART), :]

    def z_copy(src, k, way, to):
        return pltpu.make_async_remote_copy(
            src_ref=src, dst_ref=part(block, k), send_sem=z_send.at[way * PIECES + k], recv_sem=z_down.at[k],
            device_id=to, device_id_type=MESH,
        )

    def z_start(q):
        @pl.when(root)
        def _():
            def one(i, carry):
                k = q * (PIECES // CHUNKS) + i
                src = gathered.at[at(k * PART, PART, PART), at(offset, COLS, COLS)]

                @pl.when(child_up)
                def _():
                    z_copy(src, k, 0, up_device).start()

                @pl.when(child_down)
                def _():
                    z_copy(src, k, 1, down_device).start()

                return carry

            lax.fori_loop(0, PIECES // CHUNKS, one, 0)

    def z_round(step):
        first = (step - SKEW * (depth - 1)) * PACK

        @pl.when(below & (first >= 0) & (first < PIECES))
        def _():
            def one(i, carry):
                k = first + i
                src = part(block, k)
                z_copy(src, k, 0, up_device).wait_recv()

                @pl.when(child_up)
                def _():
                    z_copy(src, k, 0, up_device).start()

                @pl.when(child_down)
                def _():
                    z_copy(src, k, 1, down_device).start()

                return carry

            lax.fori_loop(0, PACK, one, 0)

    def sum_copy(k, which):
        return pltpu.make_async_remote_copy(
            src_ref=part(side_sum, k), dst_ref=part(upper_in, k, which * PIECES * PART),
            send_sem=z_send.at[2 * PIECES + k], recv_sem=z_up.at[which * PIECES + k],
            device_id=(sum_above, col, rep), device_id_type=MESH,
        )

    def owner_copy(k, i):
        c = lax.rem(k, WIDE // PART) * (PART // 8) + i
        q = lax.div(k, WIDE // PART)
        return c, q, pltpu.make_async_remote_copy(
            src_ref=side_sum.at[at(k * PART + i * 8, 8, 8), :],
            dst_ref=in_root.at[at(q * 8, 8, 8), at(offset, COLS, COLS)],
            send_sem=root_send.at[k * (PART // 8) + i], recv_sem=root_recv.at[q * 4 + lax.rem(me, 4)],
            device_id=(row, lax.div(c, 8), lax.rem(c, 8)), device_id_type=MESH,
        )

    def to_owners(k):
        def one(i, carry):
            c, q, out_copy = owner_copy(k, i)

            @pl.when(c != me)
            def _():
                out_copy.start()

            @pl.when(c == me)
            def _():
                in_root[at(q * 8, 8, 8), at(offset, COLS, COLS)] = side_sum[at(k * PART + i * 8, 8, 8), :]

            return carry

        lax.fori_loop(0, PART // 8, one, 0)

    def side_copy(q):
        rows = pl.ds(q * WIDE, WIDE)
        return pltpu.make_async_remote_copy(
            src_ref=upper_sum.at[rows, :], dst_ref=side_sum.at[rows, :], send_sem=side_send.at[q],
            recv_sem=side_recv.at[q], device_id=partner, device_id_type=MESH,
        )

    def hand_over(q):
        @pl.when(active)
        def _():
            side_copy(q).start()

    def take_over(q):
        @pl.when(sum_active)
        def _():
            side_copy(q).wait_recv()

    def sum_round(step):
        first = (step - SKEW * (DEPTH - sum_depth)) * PACK

        @pl.when((sum_active | sum_relay) & (first >= 0) & (first < PIECES))
        def _():
            def one(i, carry):
                k = first + i
                for which, there in enumerate((sum_up, sum_down)):
                    @pl.when(there)
                    def _():
                        sum_copy(k, which).wait_recv()
                        mine = at(k * PART, PART, PART)
                        other = at(which * PIECES * PART + k * PART, PART, PART)
                        side_sum[mine, :] = side_sum[mine, :] + upper_in[other, :]

                @pl.when(sum_below)
                def _():
                    sum_copy(k, sum_slot).start()

                @pl.when(sum_root)
                def _():
                    to_owners(k)

                return carry

            lax.fori_loop(0, PACK, one, 0)

    def prepare():
        def one(n, carry):
            rows = at(n * 256, 256, 256)
            pltpu.make_async_copy(upstream.at[rows, :], tile.at[rows, :], local_sem.at[n]).wait()
            row_number = row * ROWS + n * 256 + lax.broadcasted_iota(jnp.int32, (256, COLS), 0)
            col_number = me * COLS + lax.broadcasted_iota(jnp.int32, (256, COLS), 1)
            kept = jnp.where(col_number <= row_number, tile[rows, :], 0.0)
            tile_high[rows, :], tile_low[rows, :] = halves(kept)
            return carry

        lax.fori_loop(0, 8, one, 0)

        @pl.when(sum_relay)
        def _():
            def clear_relay(n, carry):
                side_sum[at(n * 64, 64, 64), :] = jnp.zeros((64, COLS), jnp.float32)
                return carry

            lax.fori_loop(0, 16, clear_relay, 0)

        @pl.when(jnp.logical_not(active))
        def _():
            def clear(n, carry):
                lower_sum[at(n * 64, 64, 64), :] = jnp.zeros((64, ROWS), jnp.float32)
                return carry

            lax.fori_loop(0, 16, clear, 0)

    def product(left_a, left_b, right_a, right_b, dims):
        dot = functools.partial(
            lax.dot_general, dimension_numbers=(dims, ((), ())), preferred_element_type=jnp.float32
        )
        return dot(left_a, right_a) + dot(left_b, right_a) + dot(left_a, right_b)

    def upper(q, n):
        @pl.when(active)
        def _():
            here = pl.ds(q * WIDE, WIDE)

            def cut(i, carry):
                cols = at(i * 256, 256, 256)
                left_high[:, cols], left_low[:, cols] = halves(gathered[here, cols])
                return carry

            if n == 0:
                lax.fori_loop(0, 8, cut, 0)
            cols = pl.ds(n * 256, 256)
            upper_sum[here, cols] = product(
                left_high[...], left_low[...], tile_high[:, cols], tile_low[:, cols], ((1,), (0,))
            )

    def lower(q, n):
        @pl.when(active)
        def _():
            here = pl.ds(q * WIDE, WIDE)
            if n == 0:
                @pl.when(root)
                def _():
                    right_high[...], right_low[...] = halves(gathered[here, at(offset, COLS, COLS)])

                @pl.when(below)
                def _():
                    right_high[...], right_low[...] = halves(block[here, :])

            def one(i, carry):
                rows = at(n * HALF + i * 256, 256, 256)
                lower_sum[here, rows] = product(
                    right_high[...], right_low[...], tile_high[rows, :], tile_low[rows, :], ((1,), (1,))
                )
                return carry

            lax.fori_loop(0, 4, one, 0)

    def scatter_partner(q, h):
        for half in range(2):
            send(
                group(lower_sum, q, half, 1 - core).at[:, columns(h)],
                in_partner.at[pl.ds((q * 2 + half) * 64, 64), columns(h)],
                2 * LANES + 2 * CHUNKS + (2 * q + h) * 2 + half, partner,
            )

    def scatter_far(q, h):
        base = LANES + (2 * q + h) * STAGES
        for half in range(2):
            came = pl.ds((q * 2 + half) * 64, 64)
            arrived(in_partner.at[came, columns(h)], 2 * LANES + 2 * CHUNKS + (2 * q + h) * 2 + half)
            mine = at(q * WIDE + half * 128 + core * 64, 64, 8)
            lower_sum[mine, columns(h)] = lower_sum[mine, columns(h)] + in_partner[came, columns(h)]
        for j in (3, 1, 2, 0):
            for way, step in enumerate((1, 3)):
                send(
                    total(q, chip(h, AWAY[j], 2), quarter(h, way)),
                    in_far.at[pl.ds((q * 8 + 2 * j + way) * 8, 8), pl.ds(h * (HALF // 2), HALF // 2)],
                    base + 2 * j + way, device(chip(h, 0, step), core),
                )

    def scatter_near(q, h):
        base = LANES + (2 * q + h) * STAGES
        for j in (3, 1, 2, 0):
            for way, step in enumerate((1, 3)):
                to = chip(h, AWAY[j], step)
                came = pl.ds((q * 8 + 2 * j + way) * 8, 8)
                came_cols = pl.ds(h * (HALF // 2), HALF // 2)
                arrived(in_far.at[came, came_cols], base + 2 * j + way)
                mine, cols = at(q * WIDE + number(to), 8, 8), quarter(h, way)
                lower_sum[mine, cols] = lower_sum[mine, cols] + in_far[came, came_cols]
                send(
                    total(q, to, columns(h)), in_near.at[came, columns(h)], base + 8 + 2 * j + way,
                    device(chip(h, 0, step), core),
                )

    def scatter_column(q, h):
        base, cols = LANES + (2 * q + h) * STAGES, columns(h)
        for j in (3, 1, 2, 0):
            mine = at(q * WIDE + number(chip(h, AWAY[j], 0)), 8, 8)
            first, second = (pl.ds((q * 8 + 2 * j + way) * 8, 8) for way in range(2))
            arrived(in_near.at[first, cols], base + 8 + 2 * j)
            arrived(in_near.at[second, cols], base + 8 + 2 * j + 1)
            lower_sum[mine, cols] = lower_sum[mine, cols] + (in_near[first, cols] + in_near[second, cols])
            if j == 3:
                for way, step in enumerate((1, 3)):
                    send(
                        total(q, chip(h, 2, 0), quarter(h, way)),
                        in_cross_far.at[pl.ds((q * 2 + way) * 8, 8), pl.ds(h * (HALF // 2), HALF // 2)],
                        base + 16 + way, device(chip(h, step, 0), core),
                    )

    def scatter_row(q, h):
        base = LANES + (2 * q + h) * STAGES
        for way, step in enumerate((1, 3)):
            to = chip(h, step, 0)
            came = pl.ds((q * 2 + way) * 8, 8)
            came_cols = pl.ds(h * (HALF // 2), HALF // 2)
            arrived(in_cross_far.at[came, came_cols], base + 16 + way)
            mine, cols = at(q * WIDE + number(to), 8, 8), quarter(h, way)
            lower_sum[mine, cols] = lower_sum[mine, cols] + in_cross_far[came, came_cols]
            send(total(q, to, columns(h)), in_cross.at[came, columns(h)], base + 18 + way, device(to, core))

    def scatter_done(q, h):
        base, cols = LANES + (2 * q + h) * STAGES, columns(h)
        first, second = (pl.ds((q * 2 + way) * 8, 8) for way in range(2))
        arrived(in_cross.at[first, cols], base + 18)
        arrived(in_cross.at[second, cols], base + 19)
        mine = at(q * WIDE + me * 8, 8, 8)
        out[pl.ds(q * 8, 8), cols] = lower_sum[mine, cols] + (in_cross[first, cols] + in_cross[second, cols])

    def summer(g):
        c = row * 4 + g
        return c + 8 - 16 * lax.rem(lax.div(c, 8), 2)

    def finish(q):
        here = pl.ds(q * 8, 8)
        for g in range(4):
            cols = pl.ds(g * COLS, COLS)

            @pl.when(me != summer(g))
            def _():
                piece = in_root.at[here, cols]
                pltpu.make_async_remote_copy(
                    src_ref=piece, dst_ref=piece, send_sem=root_send.at[0], recv_sem=root_recv.at[q * 4 + g],
                    device_id=partner, device_id_type=MESH,
                ).wait_recv()

        out[here, :] = out[here, :] + in_root[here, :]

    def fetch(n, carry):
        rows = at(n * 256, 256, 256)
        pltpu.make_async_copy(upstream.at[rows, :], tile.at[rows, :], local_sem.at[n]).start()
        return carry

    lax.fori_loop(0, 8, fetch, 0)
    for q in range(CHUNKS):
        gathered[at(q * WIDE + me * 8, 8, 8), :] = panel[pl.ds(q * 8, 8), :]

    barrier = pltpu.get_barrier_semaphore()

    def greet(to):
        pl.semaphore_signal(barrier, inc=1, device_id=to, device_id_type=MESH)

    for first, second in ((1, 0), (3, 0), (0, 1), (0, 3)):
        greet(device(chip(0, first, second), core))
    greet(partner)
    met = (below, child_up, child_down, sum_below, sum_up, sum_down)
    rows_met = (above, row + 1, down, sum_above, row + 1, sum_below_row)
    for there, to_row in zip(met, rows_met):
        @pl.when(there)
        def _():
            greet((to_row, col, rep))

    for g in range(4):
        @pl.when(me != summer(g))
        def _():
            c = summer(g)
            greet((row, lax.div(c, 8), lax.rem(c, 8)))

    pl.semaphore_wait(
        barrier, 5 + jnp.where(sum_root, 31, 0) + sum(jnp.where(there, 1, 0) for there in met)
    )

    tasks = locals()
    for which, *args in ORDER:
        tasks[TASKS[which]](*args)

    for one in sent:
        one.wait_send()

    def settle(k, carry):
        if True:
            @pl.when(child_up)
            def _():
                z_copy(part(block, k), k, 0, up_device).wait_send()

            @pl.when(child_down)
            def _():
                z_copy(part(block, k), k, 1, down_device).wait_send()

        if True:
            @pl.when(sum_below)
            def _():
                sum_copy(k, 0).wait_send()

            @pl.when(sum_root)
            def _():
                for i in range(PART // 8):
                    c, _, out_copy = owner_copy(k, i)

                    @pl.when(c != me)
                    def _():
                        out_copy.wait_send()

        return carry

    lax.fori_loop(0, PIECES, settle, 0)
    for q in range(CHUNKS):
        @pl.when(active)
        def _():
            side_copy(q).wait_send()


TASKS = (
    "gather_own",
    "prepare",
    "gather_first",
    "gather_opposite",
    "gather_forward",
    "gather_last",
    "gather_done",
    "z_start",
    "upper",
    "z_round",
    "hand_over",
    "take_over",
    "sum_round",
    "lower",
    "scatter_partner",
    "scatter_far",
    "scatter_near",
    "scatter_column",
    "scatter_row",
    "scatter_done",
    "finish",
)
ORDER = (
    (0, 0), (1,), (2, 0), (0, 1), (3, 0), (4, 0, 0), (4, 0, 1), (4, 0, 2), (2, 1), (4, 0, 3), (4, 1, 0),
    (0, 2), (3, 1), (5, 0), (2, 2), (4, 1, 2), (4, 1, 1), (4, 1, 3), (6, 0), (7, 0), (8, 0, 0), (0, 3),
    (3, 2), (8, 0, 1), (4, 2, 0), (9, 0), (9, 1), (10, 0), (4, 2, 1), (5, 1), (11, 0), (9, 2), (2, 3),
    (12, 0), (9, 3), (4, 2, 3), (12, 1), (4, 2, 2), (6, 1), (9, 4), (8, 1, 0), (12, 2), (9, 5), (9, 6),
    (7, 1), (8, 1, 1), (12, 3), (12, 4), (3, 3), (4, 3, 0), (4, 3, 2), (9, 7), (4, 3, 1), (10, 1), (9, 8),
    (12, 5), (5, 2), (9, 9), (12, 6), (9, 10), (12, 7), (9, 11), (6, 2), (11, 1), (12, 8), (9, 12), (4, 3, 3),
    (8, 2, 0), (9, 13), (12, 9), (12, 10), (7, 2), (8, 2, 1), (9, 14), (12, 11), (5, 3), (9, 15), (9, 16),
    (12, 12), (10, 2), (6, 3), (12, 13), (9, 17), (7, 3), (8, 3, 0), (9, 18), (12, 14), (9, 19), (11, 2),
    (12, 15), (13, 0, 0), (12, 16), (14, 0, 0), (9, 20), (9, 21), (8, 3, 1), (12, 17), (9, 22), (12, 18),
    (13, 0, 1), (14, 0, 1), (9, 23), (12, 19), (15, 0, 0), (9, 24), (10, 3), (9, 25), (12, 20), (15, 0, 1),
    (9, 26), (12, 21), (16, 0, 0), (12, 22), (9, 27), (13, 1, 0), (9, 28), (14, 1, 0), (12, 23), (11, 3),
    (9, 29), (16, 0, 1), (12, 24), (13, 1, 1), (9, 30), (15, 1, 0), (14, 1, 1), (9, 31), (12, 25), (17, 0, 0),
    (9, 32), (12, 26), (9, 33), (12, 27), (15, 1, 1), (9, 34), (16, 1, 0), (12, 28), (17, 0, 1), (9, 35),
    (13, 2, 0), (9, 36), (18, 0, 0), (12, 29), (14, 2, 0), (12, 30), (16, 1, 1), (9, 37), (13, 2, 1),
    (14, 2, 1), (9, 38), (15, 2, 0), (9, 39), (12, 31), (12, 32), (17, 1, 0), (18, 0, 1), (9, 40), (12, 33),
    (15, 2, 1), (17, 1, 1), (9, 41), (12, 34), (9, 42), (16, 2, 0), (9, 43), (12, 35), (13, 3, 0), (14, 3, 0),
    (12, 36), (18, 1, 0), (16, 2, 1), (13, 3, 1), (12, 37), (14, 3, 1), (12, 38), (15, 3, 0), (15, 3, 1),
    (18, 1, 1), (19, 1, 0), (17, 2, 0), (12, 39), (19, 0, 1), (19, 0, 0), (12, 40), (17, 2, 1), (12, 41),
    (16, 3, 0), (16, 3, 1), (12, 42), (12, 43), (18, 2, 1), (12, 44), (17, 3, 0), (17, 3, 1), (18, 2, 0),
    (12, 45), (12, 46), (18, 3, 0), (18, 3, 1), (19, 2, 0), (19, 2, 1), (19, 1, 1), (20, 1), (20, 0),
    (19, 3, 0), (20, 2), (19, 3, 1), (20, 3),
)


def per_device(upstream, input_panel):
    f32, bf16 = jnp.float32, jnp.bfloat16
    total = CHUNKS * WIDE
    vmem = pltpu.VMEM
    result = pl.pallas_call(
        kernel,
        out_shape=jax.ShapeDtypeStruct((32, ROWS), f32),
        in_specs=[pl.BlockSpec(memory_space=pl.ANY), pl.BlockSpec(memory_space=pltpu.VMEM)],
        out_specs=pl.BlockSpec(memory_space=pltpu.VMEM),
        scratch_shapes=[
            vmem((total, ROWS), f32),
            vmem((total, COLS), f32),
            vmem((total, COLS), f32),
            vmem((total, COLS), f32),
            vmem((2 * total, COLS), f32),
            vmem((total, ROWS), f32),
            vmem((total // 2, ROWS), f32),
            vmem((CHUNKS * 64, HALF), f32),
            vmem((CHUNKS * 64, ROWS), f32),
            vmem((CHUNKS * 16, HALF), f32),
            vmem((CHUNKS * 16, ROWS), f32),
            vmem((CHUNKS * 8, ROWS), f32),
            vmem((ROWS, COLS), f32),
            vmem((ROWS, COLS), bf16),
            vmem((ROWS, COLS), bf16),
            vmem((WIDE, ROWS), bf16),
            vmem((WIDE, ROWS), bf16),
            vmem((WIDE, COLS), bf16),
            vmem((WIDE, COLS), bf16),
            pltpu.SemaphoreType.DMA((COPIES,)),
            pltpu.SemaphoreType.DMA((COPIES,)),
            pltpu.SemaphoreType.DMA((3 * PIECES,)),
            pltpu.SemaphoreType.DMA((PIECES,)),
            pltpu.SemaphoreType.DMA((2 * PIECES,)),
            pltpu.SemaphoreType.DMA((PIECES * PART // 8,)),
            pltpu.SemaphoreType.DMA((CHUNKS * 4,)),
            pltpu.SemaphoreType.DMA((CHUNKS,)),
            pltpu.SemaphoreType.DMA((CHUNKS,)),
            pltpu.SemaphoreType.DMA((8,)),
        ],
        compiler_params=pltpu.CompilerParams(
            collective_id=0, has_side_effects=True, vmem_limit_bytes=60 * 1024 * 1024
        ),
    )(upstream, input_panel.T)
    return result.T


def solution(mesh):
    placed = (P("row", ("col", "rep")), P("row", ("col", "rep")))
    return jax.shard_map(
        per_device, mesh=mesh, in_specs=placed, out_specs=P("row", ("col", "rep")), check_vma=False
    )
```

```python
import functools

import jax
import jax.numpy as jnp
from jax import lax
from jax.experimental import pallas as pl
from jax.experimental.pallas import tpu as pltpu
from jax.sharding import PartitionSpec as P

MESH = pl.DeviceIdType.MESH
ROWS = 2048
COLS = 512
HALF = ROWS // 2
CHUNKS = 4
WIDE = 256
PIECES = 32
PART = 32
PACK = 1
DEPTH = 5
SKEW = 3
AWAY = (0, 3, 1, 2)
LAG = 40
STAGES = 20
LANES = 2 * CHUNKS * STAGES
COPIES = 2 * LANES + 6 * CHUNKS


def at(start, length, step):
    return pl.ds(pl.multiple_of(start, step), length)


def halves(x):
    high = x.astype(jnp.bfloat16)
    return high, (x - high.astype(jnp.float32)).astype(jnp.bfloat16)


def kernel(
    upstream, panel, out,
    gathered, block, upper_sum, side_sum, upper_in, lower_sum,
    in_partner, in_far, in_near, in_cross_far, in_cross, in_root,
    tile, tile_high, tile_low, left_high, left_low, right_high, right_low,
    send_sem, recv_sem, z_send, z_down, z_up, root_send, root_recv, side_send, side_recv, local_sem,
):
    row, col, rep = lax.axis_index("row"), lax.axis_index("col"), lax.axis_index("rep")
    core, x = lax.rem(col, 2), lax.div(rep, 2)
    y = lax.rem(rep, 2) * 2 + lax.div(col, 2)
    me = col * 8 + rep

    xs = [x] + [lax.rem(x + d, 4) for d in (1, 2, 3)]
    ys = [y] + [lax.rem(y + d, 4) for d in (1, 2, 3)]
    cols = [lax.rem(v, 2) * 2 for v in ys]
    reps = [[u * 2 + lax.div(v, 2) for v in ys] for u in xs]
    mine_at = [[((cols[b] + core) * 8 + reps[a][b]) * 8 for b in range(4)] for a in range(4)]

    def chip(order, first, second):
        return (first, second) if order == 0 else (second, first)

    def number(place):
        return mine_at[place[0]][place[1]]

    def device(place, on):
        return (row, cols[place[1]] + on, reps[place[0]][place[1]])

    low = lax.div(col, 2) * 4 + lax.div(x, 2)
    high = low + 2
    offset = lax.rem(me, 4) * COLS

    def line(first):
        second = jnp.logical_not(first)
        source = jnp.where(first, low, high)
        relay = first & (low == 4) & (row == 2)
        root, active = row == source, row >= source
        upward = second | (row <= high)
        child_up = (first & (row >= low) & (row < high)) | (second & (row >= high) & (row < 7))
        child_down = (first & ((root & (high < 7)) | (row > high + 1))) | relay
        depth = jnp.where(relay, 1, jnp.where(upward, row - source, 8 - row + jnp.where(low == 4, 1, 0)))
        far = jnp.where(row < 7, row + 1, jnp.where(low == 4, 2, low))
        above = jnp.where(relay, 4, jnp.where(upward, row - 1, far))
        down = jnp.where(root & (low == 4), 2, jnp.where(root | relay, 7, row - 1))
        slot = jnp.where(upward & jnp.logical_not(relay), 0, 1)
        return root, active, relay, active & jnp.logical_not(root) | relay, child_up, child_down, depth, above, down, slot

    root, active, _, below, child_up, child_down, depth, above, down, _ = line(core == 0)
    sum_root, sum_active, sum_relay, sum_below, sum_up, sum_down, sum_depth, sum_above, sum_below_row, sum_slot = line(core == 1)
    up_device = (row + 1, col, rep)
    down_device = (down, col, rep)
    above_device = (above, col, rep)

    def copy(src, dst, which, to):
        return pltpu.make_async_remote_copy(
            src_ref=src, dst_ref=dst, send_sem=send_sem.at[which], recv_sem=recv_sem.at[which],
            device_id=to, device_id_type=MESH,
        )

    sent = []

    def send(src, dst, which, to):
        one = copy(src, dst, which, to)
        one.start()
        sent.append(one)

    partner = (row, col + 1 - 2 * core, rep)

    def arrived(dst, which):
        copy(dst, dst, which, partner).wait_recv()

    def columns(h):
        return pl.ds(h * HALF, HALF)

    def quarter(h, way):
        return pl.ds(h * HALF + way * (HALF // 2), HALF // 2)

    def slab(q, place, cols):
        return gathered.at[at(q * WIDE + number(place), 8, 8), cols]

    def total(q, place, cols):
        return lower_sum.at[at(q * WIDE + number(place), 8, 8), cols]

    def group(ref, q, half, on):
        return ref.at[at(q * WIDE + half * 128 + on * 64, 64, 8), :]

    def gather_own(q):
        own = panel.at[pl.ds(q * 8, 8), :]
        for axis in range(2):
            for h in range(2):
                base, cols = (2 * q + h) * STAGES, columns(h)
                for way, step in enumerate((1, 3)):
                    to = chip(h, step, 0) if axis == 0 else chip(h, 0, step)
                    send(own.at[:, cols], slab(q, (0, 0), cols), base + (0 if axis == 0 else 4) + way, device(to, core))

    def gather_across(q, h, j):
        base = (2 * q + h) * STAGES + 4 + 2 * j
        piece = slab(q, chip(h, AWAY[j], 0), columns(h))
        send(piece, piece, base + 0, device(chip(h, 0, 1), core))
        send(piece, piece, base + 1, device(chip(h, 0, 3), core))

    def gather_first(q):
        for h in range(2):
            base = (2 * q + h) * STAGES
            arrived(slab(q, chip(h, 3, 0), columns(h)), base + 0)
            piece = slab(q, chip(h, 3, 0), quarter(h, 0))
            send(piece, piece, base + 2, device(chip(h, 1, 0), core))
            arrived(slab(q, chip(h, 1, 0), columns(h)), base + 1)
            piece = slab(q, chip(h, 1, 0), quarter(h, 1))
            send(piece, piece, base + 3, device(chip(h, 3, 0), core))
        for h in range(2):
            gather_across(q, h, 1)
            gather_across(q, h, 2)

    def gather_opposite(q):
        for h in range(2):
            base = (2 * q + h) * STAGES
            arrived(slab(q, chip(h, 2, 0), quarter(h, 0)), base + 2)
            arrived(slab(q, chip(h, 2, 0), quarter(h, 1)), base + 3)
            gather_across(q, h, 3)

    def gather_forward(q, j):
        for h in range(2):
            base = (2 * q + h) * STAGES + 4 + 2 * j
            arrived(slab(q, chip(h, AWAY[j], 3), columns(h)), base + 0)
            piece = slab(q, chip(h, AWAY[j], 3), quarter(h, 0))
            send(piece, piece, base + 8, device(chip(h, 0, 1), core))
            arrived(slab(q, chip(h, AWAY[j], 1), columns(h)), base + 1)
            piece = slab(q, chip(h, AWAY[j], 1), quarter(h, 1))
            send(piece, piece, base + 9, device(chip(h, 0, 3), core))

    def gather_last(q):
        for h in range(2):
            base = (2 * q + h) * STAGES + 12
            for j in range(4):
                arrived(slab(q, chip(h, AWAY[j], 2), quarter(h, 0)), base + 2 * j)
                arrived(slab(q, chip(h, AWAY[j], 2), quarter(h, 1)), base + 2 * j + 1)
        for half in range(2):
            piece = group(gathered, q, half, core)
            send(piece, piece, 2 * LANES + 2 * q + half, partner)

    def gather_done(q):
        for half in range(2):
            arrived(group(gathered, q, half, 1 - core), 2 * LANES + 2 * q + half)

    def part(ref, k, more=0):
        return ref.at[at(more + k * PART, PART, PART), :]

    def z_copy(src, k, way, to):
        return pltpu.make_async_remote_copy(
            src_ref=src, dst_ref=part(block, k), send_sem=z_send.at[way * PIECES + k], recv_sem=z_down.at[k],
            device_id=to, device_id_type=MESH,
        )

    def z_start(q):
        @pl.when(root)
        def _():
            def one(i, carry):
                k = q * (PIECES // CHUNKS) + i
                src = gathered.at[at(k * PART, PART, PART), at(offset, COLS, COLS)]

                @pl.when(child_up)
                def _():
                    z_copy(src, k, 0, up_device).start()

                @pl.when(child_down)
                def _():
                    z_copy(src, k, 1, down_device).start()

                return carry

            lax.fori_loop(0, PIECES // CHUNKS, one, 0)

    def z_round(step):
        first = (step - SKEW * (depth - 1)) * PACK

        @pl.when(below & (first >= 0) & (first < PIECES))
        def _():
            def one(i, carry):
                k = first + i
                src = part(block, k)
                z_copy(src, k, 0, up_device).wait_recv()

                @pl.when(child_up)
                def _():
                    z_copy(src, k, 0, up_device).start()

                @pl.when(child_down)
                def _():
                    z_copy(src, k, 1, down_device).start()

                return carry

            lax.fori_loop(0, PACK, one, 0)

    def sum_copy(k, which):
        return pltpu.make_async_remote_copy(
            src_ref=part(side_sum, k), dst_ref=part(upper_in, k, which * PIECES * PART),
            send_sem=z_send.at[2 * PIECES + k], recv_sem=z_up.at[which * PIECES + k],
            device_id=(sum_above, col, rep), device_id_type=MESH,
        )

    def owner_copy(k, i):
        c = lax.rem(k, WIDE // PART) * (PART // 8) + i
        q = lax.div(k, WIDE // PART)
        return c, q, pltpu.make_async_remote_copy(
            src_ref=side_sum.at[at(k * PART + i * 8, 8, 8), :],
            dst_ref=in_root.at[at(q * 8, 8, 8), at(offset, COLS, COLS)],
            send_sem=root_send.at[k * (PART // 8) + i], recv_sem=root_recv.at[q * 4 + lax.rem(me, 4)],
            device_id=(row, lax.div(c, 8), lax.rem(c, 8)), device_id_type=MESH,
        )

    def to_owners(k):
        def one(i, carry):
            c, q, out_copy = owner_copy(k, i)

            @pl.when(c != me)
            def _():
                out_copy.start()

            @pl.when(c == me)
            def _():
                in_root[at(q * 8, 8, 8), at(offset, COLS, COLS)] = side_sum[at(k * PART + i * 8, 8, 8), :]

            return carry

        lax.fori_loop(0, PART // 8, one, 0)

    def side_copy(q):
        rows = pl.ds(q * WIDE, WIDE)
        return pltpu.make_async_remote_copy(
            src_ref=upper_sum.at[rows, :], dst_ref=side_sum.at[rows, :], send_sem=side_send.at[q],
            recv_sem=side_recv.at[q], device_id=partner, device_id_type=MESH,
        )

    def hand_over(q):
        @pl.when(active)
        def _():
            side_copy(q).start()

    def take_over(q):
        @pl.when(sum_active)
        def _():
            side_copy(q).wait_recv()

    def sum_round(step):
        first = (step - SKEW * (DEPTH - sum_depth)) * PACK

        @pl.when((sum_active | sum_relay) & (first >= 0) & (first < PIECES))
        def _():
            def one(i, carry):
                k = first + i
                for which, there in enumerate((sum_up, sum_down)):
                    @pl.when(there)
                    def _():
                        sum_copy(k, which).wait_recv()
                        mine = at(k * PART, PART, PART)
                        other = at(which * PIECES * PART + k * PART, PART, PART)
                        side_sum[mine, :] = side_sum[mine, :] + upper_in[other, :]

                @pl.when(sum_below)
                def _():
                    sum_copy(k, sum_slot).start()

                @pl.when(sum_root)
                def _():
                    to_owners(k)

                return carry

            lax.fori_loop(0, PACK, one, 0)

    def prepare():
        def one(n, carry):
            rows = at(n * 256, 256, 256)
            pltpu.make_async_copy(upstream.at[rows, :], tile.at[rows, :], local_sem.at[n]).wait()
            row_number = row * ROWS + n * 256 + lax.broadcasted_iota(jnp.int32, (256, COLS), 0)
            col_number = me * COLS + lax.broadcasted_iota(jnp.int32, (256, COLS), 1)
            kept = jnp.where(col_number <= row_number, tile[rows, :], 0.0)
            tile_high[rows, :], tile_low[rows, :] = halves(kept)
            return carry

        lax.fori_loop(0, 8, one, 0)

        @pl.when(sum_relay)
        def _():
            def clear_relay(n, carry):
                side_sum[at(n * 64, 64, 64), :] = jnp.zeros((64, COLS), jnp.float32)
                return carry

            lax.fori_loop(0, 16, clear_relay, 0)

        @pl.when(jnp.logical_not(active))
        def _():
            def clear(n, carry):
                lower_sum[at(n * 64, 64, 64), :] = jnp.zeros((64, ROWS), jnp.float32)
                return carry

            lax.fori_loop(0, 16, clear, 0)

    def product(left_a, left_b, right_a, right_b, dims):
        dot = functools.partial(
            lax.dot_general, dimension_numbers=(dims, ((), ())), preferred_element_type=jnp.float32
        )
        return dot(left_a, right_a) + dot(left_b, right_a) + dot(left_a, right_b)

    def upper(q, n):
        @pl.when(active)
        def _():
            here = pl.ds(q * WIDE, WIDE)

            def cut(i, carry):
                cols = at(i * 256, 256, 256)
                left_high[:, cols], left_low[:, cols] = halves(gathered[here, cols])
                return carry

            if n == 0:
                lax.fori_loop(0, 8, cut, 0)
            cols = pl.ds(n * 256, 256)
            upper_sum[here, cols] = product(
                left_high[...], left_low[...], tile_high[:, cols], tile_low[:, cols], ((1,), (0,))
            )

    def lower(q, n):
        @pl.when(active)
        def _():
            here = pl.ds(q * WIDE, WIDE)
            if n == 0:
                @pl.when(root)
                def _():
                    right_high[...], right_low[...] = halves(gathered[here, at(offset, COLS, COLS)])

                @pl.when(below)
                def _():
                    right_high[...], right_low[...] = halves(block[here, :])

            def one(i, carry):
                rows = at(n * HALF + i * 256, 256, 256)
                lower_sum[here, rows] = product(
                    right_high[...], right_low[...], tile_high[rows, :], tile_low[rows, :], ((1,), (1,))
                )
                return carry

            lax.fori_loop(0, 4, one, 0)

    def scatter_partner(q, h):
        for half in range(2):
            send(
                group(lower_sum, q, half, 1 - core).at[:, columns(h)],
                in_partner.at[pl.ds((q * 2 + half) * 64, 64), columns(h)],
                2 * LANES + 2 * CHUNKS + (2 * q + h) * 2 + half, partner,
            )

    def scatter_far(q, h):
        base = LANES + (2 * q + h) * STAGES
        for half in range(2):
            came = pl.ds((q * 2 + half) * 64, 64)
            arrived(in_partner.at[came, columns(h)], 2 * LANES + 2 * CHUNKS + (2 * q + h) * 2 + half)
            mine = at(q * WIDE + half * 128 + core * 64, 64, 8)
            lower_sum[mine, columns(h)] = lower_sum[mine, columns(h)] + in_partner[came, columns(h)]
        for j in (3, 1, 2, 0):
            for way, step in enumerate((1, 3)):
                send(
                    total(q, chip(h, AWAY[j], 2), quarter(h, way)),
                    in_far.at[pl.ds((q * 8 + 2 * j + way) * 8, 8), pl.ds(h * (HALF // 2), HALF // 2)],
                    base + 2 * j + way, device(chip(h, 0, step), core),
                )

    def scatter_near(q, h):
        base = LANES + (2 * q + h) * STAGES
        for j in (3, 1, 2, 0):
            for way, step in enumerate((1, 3)):
                to = chip(h, AWAY[j], step)
                came = pl.ds((q * 8 + 2 * j + way) * 8, 8)
                came_cols = pl.ds(h * (HALF // 2), HALF // 2)
                arrived(in_far.at[came, came_cols], base + 2 * j + way)
                mine, cols = at(q * WIDE + number(to), 8, 8), quarter(h, way)
                lower_sum[mine, cols] = lower_sum[mine, cols] + in_far[came, came_cols]
                send(
                    total(q, to, columns(h)), in_near.at[came, columns(h)], base + 8 + 2 * j + way,
                    device(chip(h, 0, step), core),
                )

    def scatter_column(q, h):
        base, cols = LANES + (2 * q + h) * STAGES, columns(h)
        for j in (3, 1, 2, 0):
            mine = at(q * WIDE + number(chip(h, AWAY[j], 0)), 8, 8)
            first, second = (pl.ds((q * 8 + 2 * j + way) * 8, 8) for way in range(2))
            arrived(in_near.at[first, cols], base + 8 + 2 * j)
            arrived(in_near.at[second, cols], base + 8 + 2 * j + 1)
            lower_sum[mine, cols] = lower_sum[mine, cols] + (in_near[first, cols] + in_near[second, cols])
            if j == 3:
                for way, step in enumerate((1, 3)):
                    send(
                        total(q, chip(h, 2, 0), quarter(h, way)),
                        in_cross_far.at[pl.ds((q * 2 + way) * 8, 8), pl.ds(h * (HALF // 2), HALF // 2)],
                        base + 16 + way, device(chip(h, step, 0), core),
                    )

    def scatter_row(q, h):
        base = LANES + (2 * q + h) * STAGES
        for way, step in enumerate((1, 3)):
            to = chip(h, step, 0)
            came = pl.ds((q * 2 + way) * 8, 8)
            came_cols = pl.ds(h * (HALF // 2), HALF // 2)
            arrived(in_cross_far.at[came, came_cols], base + 16 + way)
            mine, cols = at(q * WIDE + number(to), 8, 8), quarter(h, way)
            lower_sum[mine, cols] = lower_sum[mine, cols] + in_cross_far[came, came_cols]
            send(total(q, to, columns(h)), in_cross.at[came, columns(h)], base + 18 + way, device(to, core))

    def scatter_done(q, h):
        base, cols = LANES + (2 * q + h) * STAGES, columns(h)
        first, second = (pl.ds((q * 2 + way) * 8, 8) for way in range(2))
        arrived(in_cross.at[first, cols], base + 18)
        arrived(in_cross.at[second, cols], base + 19)
        mine = at(q * WIDE + me * 8, 8, 8)
        out[pl.ds(q * 8, 8), cols] = lower_sum[mine, cols] + (in_cross[first, cols] + in_cross[second, cols])

    def summer(g):
        c = row * 4 + g
        return c + 8 - 16 * lax.rem(lax.div(c, 8), 2)

    def finish(q):
        here = pl.ds(q * 8, 8)
        for g in range(4):
            cols = pl.ds(g * COLS, COLS)

            @pl.when(me != summer(g))
            def _():
                piece = in_root.at[here, cols]
                pltpu.make_async_remote_copy(
                    src_ref=piece, dst_ref=piece, send_sem=root_send.at[0], recv_sem=root_recv.at[q * 4 + g],
                    device_id=partner, device_id_type=MESH,
                ).wait_recv()

        out[here, :] = out[here, :] + in_root[here, :]

    barrier = pltpu.get_barrier_semaphore()

    def greet(to):
        pl.semaphore_signal(barrier, inc=1, device_id=to, device_id_type=MESH)

    for first, second in ((1, 0), (3, 0), (0, 1), (0, 3)):
        greet(device(chip(0, first, second), core))
    greet(partner)
    met = (below, child_up, child_down, sum_below, sum_up, sum_down)
    rows_met = (above, row + 1, down, sum_above, row + 1, sum_below_row)
    for there, to_row in zip(met, rows_met):
        @pl.when(there)
        def _():
            greet((to_row, col, rep))

    for g in range(4):
        @pl.when(me != summer(g))
        def _():
            c = summer(g)
            greet((row, lax.div(c, 8), lax.rem(c, 8)))

    def fetch(n, carry):
        rows = at(n * 256, 256, 256)
        pltpu.make_async_copy(upstream.at[rows, :], tile.at[rows, :], local_sem.at[n]).start()
        return carry

    lax.fori_loop(0, 8, fetch, 0)
    for q in range(CHUNKS):
        gathered[at(q * WIDE + me * 8, 8, 8), :] = panel[pl.ds(q * 8, 8), :]

    pl.semaphore_wait(
        barrier, 5 + jnp.where(sum_root, 31, 0) + sum(jnp.where(there, 1, 0) for there in met)
    )

    def settle_down(k, carry):
        @pl.when(child_up)
        def _():
            z_copy(part(block, k), k, 0, up_device).wait_send()

        @pl.when(child_down)
        def _():
            z_copy(part(block, k), k, 1, down_device).wait_send()

        return carry

    def settle_sum(k, carry):
        @pl.when(sum_below)
        def _():
            sum_copy(k, 0).wait_send()

        @pl.when(sum_root)
        def _():
            for i in range(PART // 8):
                c, _, out_copy = owner_copy(k, i)

                @pl.when(c != me)
                def _():
                    out_copy.wait_send()

        return carry

    early_pieces = PIECES - PIECES // CHUNKS
    last_round = PIECES // PACK + SKEW * DEPTH - 1
    tasks = locals()
    started, settled = [], 0
    for n, (which, *args) in enumerate(ORDER):
        tasks[TASKS[which]](*args)
        started += [n] * (len(sent) - len(started))
        while settled < len(sent) and started[settled] < n - LAG:
            sent[settled].wait_send()
            settled += 1
        if TASKS[which] == "sum_round" and args[0] == last_round - 1:
            lax.fori_loop(0, PIECES, settle_down, 0)
            lax.fori_loop(0, early_pieces, settle_sum, 0)
            for q in range(CHUNKS):
                @pl.when(active)
                def _():
                    side_copy(q).wait_send()

    for one in sent[settled:]:
        one.wait_send()
    lax.fori_loop(early_pieces, PIECES, settle_sum, 0)


TASKS = (
    "gather_own",
    "prepare",
    "gather_first",
    "gather_opposite",
    "gather_forward",
    "gather_last",
    "gather_done",
    "z_start",
    "upper",
    "z_round",
    "hand_over",
    "take_over",
    "sum_round",
    "lower",
    "scatter_partner",
    "scatter_far",
    "scatter_near",
    "scatter_column",
    "scatter_row",
    "scatter_done",
    "finish",
)
ORDER = (
    (0, 0), (1,), (2, 0), (0, 1), (3, 0), (4, 0, 0), (4, 0, 1), (4, 0, 2), (2, 1), (4, 0, 3), (4, 1, 0),
    (0, 2), (3, 1), (5, 0), (2, 2), (4, 1, 2), (4, 1, 1), (4, 1, 3), (6, 0), (7, 0), (8, 0, 0), (0, 3),
    (3, 2), (8, 0, 1), (4, 2, 0), (9, 0), (9, 1), (10, 0), (4, 2, 1), (5, 1), (11, 0), (9, 2), (2, 3),
    (12, 0), (9, 3), (4, 2, 3), (12, 1), (4, 2, 2), (6, 1), (9, 4), (8, 1, 0), (12, 2), (9, 5), (9, 6),
    (7, 1), (8, 1, 1), (12, 3), (12, 4), (3, 3), (4, 3, 0), (4, 3, 2), (9, 7), (4, 3, 1), (10, 1), (9, 8),
    (12, 5), (5, 2), (9, 9), (12, 6), (9, 10), (12, 7), (9, 11), (6, 2), (11, 1), (12, 8), (9, 12), (4, 3, 3),
    (8, 2, 0), (9, 13), (12, 9), (12, 10), (7, 2), (8, 2, 1), (9, 14), (12, 11), (5, 3), (9, 15), (9, 16),
    (12, 12), (10, 2), (6, 3), (12, 13), (9, 17), (7, 3), (8, 3, 0), (9, 18), (12, 14), (9, 19), (11, 2),
    (12, 15), (13, 0, 0), (12, 16), (14, 0, 0), (9, 20), (9, 21), (8, 3, 1), (12, 17), (9, 22), (12, 18),
    (13, 0, 1), (14, 0, 1), (9, 23), (12, 19), (15, 0, 0), (9, 24), (10, 3), (9, 25), (12, 20), (15, 0, 1),
    (9, 26), (12, 21), (16, 0, 0), (12, 22), (9, 27), (13, 1, 0), (9, 28), (14, 1, 0), (12, 23), (11, 3),
    (9, 29), (16, 0, 1), (12, 24), (13, 1, 1), (9, 30), (15, 1, 0), (14, 1, 1), (9, 31), (12, 25), (17, 0, 0),
    (9, 32), (12, 26), (9, 33), (12, 27), (15, 1, 1), (9, 34), (16, 1, 0), (12, 28), (17, 0, 1), (9, 35),
    (13, 2, 0), (9, 36), (18, 0, 0), (12, 29), (14, 2, 0), (12, 30), (16, 1, 1), (9, 37), (13, 2, 1),
    (14, 2, 1), (9, 38), (15, 2, 0), (9, 39), (12, 31), (12, 32), (17, 1, 0), (18, 0, 1), (9, 40), (12, 33),
    (15, 2, 1), (17, 1, 1), (9, 41), (12, 34), (9, 42), (16, 2, 0), (9, 43), (12, 35), (13, 3, 0), (14, 3, 0),
    (12, 36), (18, 1, 0), (16, 2, 1), (13, 3, 1), (12, 37), (14, 3, 1), (12, 38), (15, 3, 0), (15, 3, 1),
    (18, 1, 1), (19, 1, 0), (17, 2, 0), (12, 39), (19, 0, 1), (19, 0, 0), (12, 40), (17, 2, 1), (12, 41),
    (16, 3, 0), (16, 3, 1), (12, 42), (12, 43), (18, 2, 1), (12, 44), (17, 3, 0), (17, 3, 1), (18, 2, 0),
    (12, 45), (12, 46), (18, 3, 0), (18, 3, 1), (19, 2, 0), (19, 2, 1), (19, 1, 1), (20, 1), (20, 0),
    (19, 3, 0), (20, 2), (19, 3, 1), (20, 3),
)


def per_device(upstream, input_panel):
    f32, bf16 = jnp.float32, jnp.bfloat16
    total = CHUNKS * WIDE
    vmem = pltpu.VMEM
    result = pl.pallas_call(
        kernel,
        out_shape=jax.ShapeDtypeStruct((32, ROWS), f32),
        in_specs=[pl.BlockSpec(memory_space=pl.ANY), pl.BlockSpec(memory_space=pltpu.VMEM)],
        out_specs=pl.BlockSpec(memory_space=pltpu.VMEM),
        scratch_shapes=[
            vmem((total, ROWS), f32),
            vmem((total, COLS), f32),
            vmem((total, COLS), f32),
            vmem((total, COLS), f32),
            vmem((2 * total, COLS), f32),
            vmem((total, ROWS), f32),
            vmem((total // 2, ROWS), f32),
            vmem((CHUNKS * 64, HALF), f32),
            vmem((CHUNKS * 64, ROWS), f32),
            vmem((CHUNKS * 16, HALF), f32),
            vmem((CHUNKS * 16, ROWS), f32),
            vmem((CHUNKS * 8, ROWS), f32),
            vmem((ROWS, COLS), f32),
            vmem((ROWS, COLS), bf16),
            vmem((ROWS, COLS), bf16),
            vmem((WIDE, ROWS), bf16),
            vmem((WIDE, ROWS), bf16),
            vmem((WIDE, COLS), bf16),
            vmem((WIDE, COLS), bf16),
            pltpu.SemaphoreType.DMA((COPIES,)),
            pltpu.SemaphoreType.DMA((COPIES,)),
            pltpu.SemaphoreType.DMA((3 * PIECES,)),
            pltpu.SemaphoreType.DMA((PIECES,)),
            pltpu.SemaphoreType.DMA((2 * PIECES,)),
            pltpu.SemaphoreType.DMA((PIECES * PART // 8,)),
            pltpu.SemaphoreType.DMA((CHUNKS * 4,)),
            pltpu.SemaphoreType.DMA((CHUNKS,)),
            pltpu.SemaphoreType.DMA((CHUNKS,)),
            pltpu.SemaphoreType.DMA((8,)),
        ],
        compiler_params=pltpu.CompilerParams(
            collective_id=0, has_side_effects=True, vmem_limit_bytes=60 * 1024 * 1024
        ),
    )(upstream, input_panel.T)
    return result.T


def solution(mesh):
    placed = (P("row", ("col", "rep")), P("row", ("col", "rep")))
    return jax.shard_map(
        per_device, mesh=mesh, in_specs=placed, out_specs=P("row", ("col", "rep")), check_vma=False
    )
```

```python
import functools

import jax
import jax.numpy as jnp
from jax import lax
from jax.experimental import pallas as pl
from jax.experimental.pallas import tpu as pltpu
from jax.sharding import PartitionSpec as P

MESH = pl.DeviceIdType.MESH
ROWS = 2048
COLS = 512
HALF = ROWS // 2
CHUNKS = 4
WIDE = 256
PIECES = 32
PART = 32
PACK = 1
DEPTH = 5
SKEW = 3
AWAY = (0, 3, 1, 2)
LAG = 40
STAGES = 20
LANES = 2 * CHUNKS * STAGES
COPIES = 2 * LANES + 6 * CHUNKS


def at(start, length, step):
    return pl.ds(pl.multiple_of(start, step), length)


def halves(x):
    high = x.astype(jnp.bfloat16)
    return high, (x - high.astype(jnp.float32)).astype(jnp.bfloat16)


def kernel(
    upstream, panel, out,
    gathered, block, upper_sum, side_sum, upper_in, lower_sum,
    in_partner, in_far, in_near, in_cross_far, in_cross, in_root,
    tile, tile_high, tile_low, left_high, left_low, right_high, right_low,
    send_sem, recv_sem, z_send, z_down, z_up, root_send, root_recv, side_send, side_recv, local_sem,
):
    row, col, rep = lax.axis_index("row"), lax.axis_index("col"), lax.axis_index("rep")
    core, x = lax.rem(col, 2), lax.div(rep, 2)
    y = lax.rem(rep, 2) * 2 + lax.div(col, 2)
    me = col * 8 + rep

    xs = [x] + [lax.rem(x + d, 4) for d in (1, 2, 3)]
    ys = [y] + [lax.rem(y + d, 4) for d in (1, 2, 3)]
    cols = [lax.rem(v, 2) * 2 for v in ys]
    reps = [[u * 2 + lax.div(v, 2) for v in ys] for u in xs]
    mine_at = [[((cols[b] + core) * 8 + reps[a][b]) * 8 for b in range(4)] for a in range(4)]

    def chip(order, first, second):
        return (first, second) if order == 0 else (second, first)

    def number(place):
        return mine_at[place[0]][place[1]]

    def device(place, on):
        return (row, cols[place[1]] + on, reps[place[0]][place[1]])

    low = lax.div(col, 2) * 4 + lax.div(x, 2)
    high = low + 2
    offset = lax.rem(me, 4) * COLS

    def line(first):
        second = jnp.logical_not(first)
        source = jnp.where(first, low, high)
        relay = first & (low == 4) & (row == 2)
        root, active = row == source, row >= source
        upward = second | (row <= high)
        child_up = (first & (row >= low) & (row < high)) | (second & (row >= high) & (row < 7))
        child_down = (first & ((root & (high < 7)) | (row > high + 1))) | relay
        depth = jnp.where(relay, 1, jnp.where(upward, row - source, 8 - row + jnp.where(low == 4, 1, 0)))
        far = jnp.where(row < 7, row + 1, jnp.where(low == 4, 2, low))
        above = jnp.where(relay, 4, jnp.where(upward, lax.rem(row + 7, 8), far))
        down = jnp.where(root & (low == 4), 2, jnp.where(root | relay, 7, lax.rem(row + 7, 8)))
        slot = jnp.where(upward & jnp.logical_not(relay), 0, 1)
        return root, active, relay, active & jnp.logical_not(root) | relay, child_up, child_down, depth, above, down, slot

    root, active, _, below, child_up, child_down, depth, above, down, _ = line(core == 0)
    sum_root, sum_active, sum_relay, sum_below, sum_up, sum_down, sum_depth, sum_above, sum_below_row, sum_slot = line(core == 1)
    up_device = (lax.rem(row + 1, 8), col, rep)
    down_device = (down, col, rep)
    above_device = (above, col, rep)

    def copy(src, dst, which, to):
        return pltpu.make_async_remote_copy(
            src_ref=src, dst_ref=dst, send_sem=send_sem.at[which], recv_sem=recv_sem.at[which],
            device_id=to, device_id_type=MESH,
        )

    sent = []

    def send(src, dst, which, to):
        one = copy(src, dst, which, to)
        one.start()
        sent.append(one)

    partner = (row, col + 1 - 2 * core, rep)

    def arrived(dst, which):
        copy(dst, dst, which, partner).wait_recv()

    def columns(h):
        return pl.ds(h * HALF, HALF)

    def quarter(h, way):
        return pl.ds(h * HALF + way * (HALF // 2), HALF // 2)

    def slab(q, place, cols):
        return gathered.at[at(q * WIDE + number(place), 8, 8), cols]

    def total(q, place, cols):
        return lower_sum.at[at(q * WIDE + number(place), 8, 8), cols]

    def group(ref, q, half, on):
        return ref.at[at(q * WIDE + half * 128 + on * 64, 64, 8), :]

    def gather_own(q):
        own = panel.at[pl.ds(q * 8, 8), :]
        for axis in range(2):
            for h in range(2):
                base, cols = (2 * q + h) * STAGES, columns(h)
                for way, step in enumerate((1, 3)):
                    to = chip(h, step, 0) if axis == 0 else chip(h, 0, step)
                    send(own.at[:, cols], slab(q, (0, 0), cols), base + (0 if axis == 0 else 4) + way, device(to, core))

    def gather_across(q, h, j):
        base = (2 * q + h) * STAGES + 4 + 2 * j
        piece = slab(q, chip(h, AWAY[j], 0), columns(h))
        send(piece, piece, base + 0, device(chip(h, 0, 1), core))
        send(piece, piece, base + 1, device(chip(h, 0, 3), core))

    def gather_first(q):
        for h in range(2):
            base = (2 * q + h) * STAGES
            arrived(slab(q, chip(h, 3, 0), columns(h)), base + 0)
            piece = slab(q, chip(h, 3, 0), quarter(h, 0))
            send(piece, piece, base + 2, device(chip(h, 1, 0), core))
            arrived(slab(q, chip(h, 1, 0), columns(h)), base + 1)
            piece = slab(q, chip(h, 1, 0), quarter(h, 1))
            send(piece, piece, base + 3, device(chip(h, 3, 0), core))
        for h in range(2):
            gather_across(q, h, 1)
            gather_across(q, h, 2)

    def gather_opposite(q):
        for h in range(2):
            base = (2 * q + h) * STAGES
            arrived(slab(q, chip(h, 2, 0), quarter(h, 0)), base + 2)
            arrived(slab(q, chip(h, 2, 0), quarter(h, 1)), base + 3)
            gather_across(q, h, 3)

    def gather_forward(q, j):
        for h in range(2):
            base = (2 * q + h) * STAGES + 4 + 2 * j
            arrived(slab(q, chip(h, AWAY[j], 3), columns(h)), base + 0)
            piece = slab(q, chip(h, AWAY[j], 3), quarter(h, 0))
            send(piece, piece, base + 8, device(chip(h, 0, 1), core))
            arrived(slab(q, chip(h, AWAY[j], 1), columns(h)), base + 1)
            piece = slab(q, chip(h, AWAY[j], 1), quarter(h, 1))
            send(piece, piece, base + 9, device(chip(h, 0, 3), core))

    def gather_last(q):
        for h in range(2):
            base = (2 * q + h) * STAGES + 12
            for j in range(4):
                arrived(slab(q, chip(h, AWAY[j], 2), quarter(h, 0)), base + 2 * j)
                arrived(slab(q, chip(h, AWAY[j], 2), quarter(h, 1)), base + 2 * j + 1)
        for half in range(2):
            piece = group(gathered, q, half, core)
            send(piece, piece, 2 * LANES + 2 * q + half, partner)

    def gather_done(q):
        for half in range(2):
            arrived(group(gathered, q, half, 1 - core), 2 * LANES + 2 * q + half)

    def part(ref, k, more=0):
        return ref.at[at(more + k * PART, PART, PART), :]

    def z_copy(src, k, way, to):
        return pltpu.make_async_remote_copy(
            src_ref=src, dst_ref=part(block, k), send_sem=z_send.at[way * PIECES + k], recv_sem=z_down.at[k],
            device_id=to, device_id_type=MESH,
        )

    def z_start(q):
        @pl.when(root)
        def _():
            def one(i, carry):
                k = q * (PIECES // CHUNKS) + i
                src = gathered.at[at(k * PART, PART, PART), at(offset, COLS, COLS)]

                @pl.when(child_up)
                def _():
                    z_copy(src, k, 0, up_device).start()

                @pl.when(child_down)
                def _():
                    z_copy(src, k, 1, down_device).start()

                return carry

            lax.fori_loop(0, PIECES // CHUNKS, one, 0)

    def z_round(step):
        first = (step - SKEW * (depth - 1)) * PACK

        @pl.when(below & (first >= 0) & (first < PIECES))
        def _():
            def one(i, carry):
                k = first + i
                src = part(block, k)
                z_copy(src, k, 0, up_device).wait_recv()

                @pl.when(child_up)
                def _():
                    z_copy(src, k, 0, up_device).start()

                @pl.when(child_down)
                def _():
                    z_copy(src, k, 1, down_device).start()

                return carry

            lax.fori_loop(0, PACK, one, 0)

    def sum_copy(k, which):
        return pltpu.make_async_remote_copy(
            src_ref=part(side_sum, k), dst_ref=part(upper_in, k, which * PIECES * PART),
            send_sem=z_send.at[2 * PIECES + k], recv_sem=z_up.at[which * PIECES + k],
            device_id=(sum_above, col, rep), device_id_type=MESH,
        )

    def owner_copy(k, i):
        c = lax.rem(k, WIDE // PART) * (PART // 8) + i
        q = lax.div(k, WIDE // PART)
        return c, q, pltpu.make_async_remote_copy(
            src_ref=side_sum.at[at(k * PART + i * 8, 8, 8), :],
            dst_ref=in_root.at[at(q * 8, 8, 8), at(offset, COLS, COLS)],
            send_sem=root_send.at[k * (PART // 8) + i], recv_sem=root_recv.at[q * 4 + lax.rem(me, 4)],
            device_id=(row, lax.div(c, 8), lax.rem(c, 8)), device_id_type=MESH,
        )

    def to_owners(k):
        def one(i, carry):
            c, q, out_copy = owner_copy(k, i)

            @pl.when(c != me)
            def _():
                out_copy.start()

            @pl.when(c == me)
            def _():
                in_root[at(q * 8, 8, 8), at(offset, COLS, COLS)] = side_sum[at(k * PART + i * 8, 8, 8), :]

            return carry

        lax.fori_loop(0, PART // 8, one, 0)

    def side_copy(q):
        rows = pl.ds(q * WIDE, WIDE)
        return pltpu.make_async_remote_copy(
            src_ref=upper_sum.at[rows, :], dst_ref=side_sum.at[rows, :], send_sem=side_send.at[q],
            recv_sem=side_recv.at[q], device_id=partner, device_id_type=MESH,
        )

    def hand_over(q):
        @pl.when(active)
        def _():
            side_copy(q).start()

    def take_over(q):
        @pl.when(sum_active)
        def _():
            side_copy(q).wait_recv()

    def sum_round(step):
        first = (step - SKEW * (DEPTH - sum_depth)) * PACK

        @pl.when((sum_active | sum_relay) & (first >= 0) & (first < PIECES))
        def _():
            def one(i, carry):
                k = first + i
                for which, there in enumerate((sum_up, sum_down)):
                    @pl.when(there)
                    def _():
                        sum_copy(k, which).wait_recv()
                        mine = at(k * PART, PART, PART)
                        other = at(which * PIECES * PART + k * PART, PART, PART)
                        side_sum[mine, :] = side_sum[mine, :] + upper_in[other, :]

                @pl.when(sum_below)
                def _():
                    sum_copy(k, sum_slot).start()

                @pl.when(sum_root)
                def _():
                    to_owners(k)

                return carry

            lax.fori_loop(0, PACK, one, 0)

    def prepare():
        def one(n, carry):
            rows = at(n * 256, 256, 256)
            pltpu.make_async_copy(upstream.at[rows, :], tile.at[rows, :], local_sem.at[n]).wait()
            row_number = row * ROWS + n * 256 + lax.broadcasted_iota(jnp.int32, (256, COLS), 0)
            col_number = me * COLS + lax.broadcasted_iota(jnp.int32, (256, COLS), 1)
            kept = jnp.where(col_number <= row_number, tile[rows, :], 0.0)
            tile_high[rows, :], tile_low[rows, :] = halves(kept)
            return carry

        lax.fori_loop(0, 8, one, 0)

        @pl.when(sum_relay)
        def _():
            def clear_relay(n, carry):
                side_sum[at(n * 64, 64, 64), :] = jnp.zeros((64, COLS), jnp.float32)
                return carry

            lax.fori_loop(0, 16, clear_relay, 0)

        @pl.when(jnp.logical_not(active))
        def _():
            def clear(n, carry):
                lower_sum[at(n * 64, 64, 64), :] = jnp.zeros((64, ROWS), jnp.float32)
                return carry

            lax.fori_loop(0, 16, clear, 0)

    def product(left_a, left_b, right_a, right_b, dims):
        dot = functools.partial(
            lax.dot_general, dimension_numbers=(dims, ((), ())), preferred_element_type=jnp.float32
        )
        return dot(left_a, right_a) + dot(left_b, right_a) + dot(left_a, right_b)

    def upper(q, n):
        @pl.when(active)
        def _():
            here = pl.ds(q * WIDE, WIDE)

            def cut(i, carry):
                cols = at(i * 256, 256, 256)
                left_high[:, cols], left_low[:, cols] = halves(gathered[here, cols])
                return carry

            if n == 0:
                lax.fori_loop(0, 8, cut, 0)
            cols = pl.ds(n * 256, 256)
            upper_sum[here, cols] = product(
                left_high[...], left_low[...], tile_high[:, cols], tile_low[:, cols], ((1,), (0,))
            )

    def lower(q, n):
        @pl.when(active)
        def _():
            here = pl.ds(q * WIDE, WIDE)
            if n == 0:
                @pl.when(root)
                def _():
                    right_high[...], right_low[...] = halves(gathered[here, at(offset, COLS, COLS)])

                @pl.when(below)
                def _():
                    right_high[...], right_low[...] = halves(block[here, :])

            def one(i, carry):
                rows = at(n * HALF + i * 256, 256, 256)
                lower_sum[here, rows] = product(
                    right_high[...], right_low[...], tile_high[rows, :], tile_low[rows, :], ((1,), (1,))
                )
                return carry

            lax.fori_loop(0, 4, one, 0)

    def scatter_partner(q, h):
        for half in range(2):
            send(
                group(lower_sum, q, half, 1 - core).at[:, columns(h)],
                in_partner.at[pl.ds((q * 2 + half) * 64, 64), columns(h)],
                2 * LANES + 2 * CHUNKS + (2 * q + h) * 2 + half, partner,
            )

    def scatter_far(q, h):
        base = LANES + (2 * q + h) * STAGES
        for half in range(2):
            came = pl.ds((q * 2 + half) * 64, 64)
            arrived(in_partner.at[came, columns(h)], 2 * LANES + 2 * CHUNKS + (2 * q + h) * 2 + half)
            mine = at(q * WIDE + half * 128 + core * 64, 64, 8)
            lower_sum[mine, columns(h)] = lower_sum[mine, columns(h)] + in_partner[came, columns(h)]
        for j in (3, 1, 2, 0):
            for way, step in enumerate((1, 3)):
                send(
                    total(q, chip(h, AWAY[j], 2), quarter(h, way)),
                    in_far.at[pl.ds((q * 8 + 2 * j + way) * 8, 8), pl.ds(h * (HALF // 2), HALF // 2)],
                    base + 2 * j + way, device(chip(h, 0, step), core),
                )

    def scatter_near(q, h):
        base = LANES + (2 * q + h) * STAGES
        for j in (3, 1, 2, 0):
            for way, step in enumerate((1, 3)):
                to = chip(h, AWAY[j], step)
                came = pl.ds((q * 8 + 2 * j + way) * 8, 8)
                came_cols = pl.ds(h * (HALF // 2), HALF // 2)
                arrived(in_far.at[came, came_cols], base + 2 * j + way)
                mine, cols = at(q * WIDE + number(to), 8, 8), quarter(h, way)
                lower_sum[mine, cols] = lower_sum[mine, cols] + in_far[came, came_cols]
                send(
                    total(q, to, columns(h)), in_near.at[came, columns(h)], base + 8 + 2 * j + way,
                    device(chip(h, 0, step), core),
                )

    def scatter_column(q, h):
        base, cols = LANES + (2 * q + h) * STAGES, columns(h)
        for j in (3, 1, 2, 0):
            mine = at(q * WIDE + number(chip(h, AWAY[j], 0)), 8, 8)
            first, second = (pl.ds((q * 8 + 2 * j + way) * 8, 8) for way in range(2))
            arrived(in_near.at[first, cols], base + 8 + 2 * j)
            arrived(in_near.at[second, cols], base + 8 + 2 * j + 1)
            lower_sum[mine, cols] = lower_sum[mine, cols] + (in_near[first, cols] + in_near[second, cols])
            if j == 3:
                for way, step in enumerate((1, 3)):
                    send(
                        total(q, chip(h, 2, 0), quarter(h, way)),
                        in_cross_far.at[pl.ds((q * 2 + way) * 8, 8), pl.ds(h * (HALF // 2), HALF // 2)],
                        base + 16 + way, device(chip(h, step, 0), core),
                    )

    def scatter_row(q, h):
        base = LANES + (2 * q + h) * STAGES
        for way, step in enumerate((1, 3)):
            to = chip(h, step, 0)
            came = pl.ds((q * 2 + way) * 8, 8)
            came_cols = pl.ds(h * (HALF // 2), HALF // 2)
            arrived(in_cross_far.at[came, came_cols], base + 16 + way)
            mine, cols = at(q * WIDE + number(to), 8, 8), quarter(h, way)
            lower_sum[mine, cols] = lower_sum[mine, cols] + in_cross_far[came, came_cols]
            send(total(q, to, columns(h)), in_cross.at[came, columns(h)], base + 18 + way, device(to, core))

    def scatter_done(q, h):
        base, cols = LANES + (2 * q + h) * STAGES, columns(h)
        first, second = (pl.ds((q * 2 + way) * 8, 8) for way in range(2))
        arrived(in_cross.at[first, cols], base + 18)
        arrived(in_cross.at[second, cols], base + 19)
        mine = at(q * WIDE + me * 8, 8, 8)
        out[pl.ds(q * 8, 8), cols] = lower_sum[mine, cols] + (in_cross[first, cols] + in_cross[second, cols])

    def summer(g):
        c = row * 4 + g
        return c + 8 - 16 * lax.rem(lax.div(c, 8), 2)

    def finish(q):
        here = pl.ds(q * 8, 8)
        for g in range(4):
            cols = pl.ds(g * COLS, COLS)

            @pl.when(me != summer(g))
            def _():
                piece = in_root.at[here, cols]
                pltpu.make_async_remote_copy(
                    src_ref=piece, dst_ref=piece, send_sem=root_send.at[0], recv_sem=root_recv.at[q * 4 + g],
                    device_id=partner, device_id_type=MESH,
                ).wait_recv()

        out[here, :] = out[here, :] + in_root[here, :]

    barrier = pltpu.get_barrier_semaphore()

    def greet(to):
        pl.semaphore_signal(barrier, inc=1, device_id=to, device_id_type=MESH)

    for first, second in ((1, 0), (3, 0), (0, 1), (0, 3)):
        greet(device(chip(0, first, second), core))
    greet(partner)
    met = (below, child_up, child_down, sum_below, sum_up, sum_down)
    rows_met = (above, up_device[0], down, sum_above, up_device[0], sum_below_row)
    for there, to_row in zip(met, rows_met):
        @pl.when(there)
        def _():
            greet((to_row, col, rep))

    for g in range(4):
        @pl.when(me != summer(g))
        def _():
            c = summer(g)
            greet((row, lax.div(c, 8), lax.rem(c, 8)))

    def fetch(n, carry):
        rows = at(n * 256, 256, 256)
        pltpu.make_async_copy(upstream.at[rows, :], tile.at[rows, :], local_sem.at[n]).start()
        return carry

    lax.fori_loop(0, 8, fetch, 0)
    for q in range(CHUNKS):
        gathered[at(q * WIDE + me * 8, 8, 8), :] = panel[pl.ds(q * 8, 8), :]

    pl.semaphore_wait(
        barrier, 5 + jnp.where(sum_root, 31, 0) + sum(jnp.where(there, 1, 0) for there in met)
    )

    def settle_down(k, carry):
        @pl.when(child_up)
        def _():
            z_copy(part(block, k), k, 0, up_device).wait_send()

        @pl.when(child_down)
        def _():
            z_copy(part(block, k), k, 1, down_device).wait_send()

        return carry

    def settle_sum(k, carry):
        @pl.when(sum_below)
        def _():
            sum_copy(k, 0).wait_send()

        @pl.when(sum_root)
        def _():
            for i in range(PART // 8):
                c, _, out_copy = owner_copy(k, i)

                @pl.when(c != me)
                def _():
                    out_copy.wait_send()

        return carry

    early_pieces = PIECES - PIECES // CHUNKS
    last_round = PIECES // PACK + SKEW * DEPTH - 1
    tasks = locals()
    started, settled = [], 0
    for n, (which, *args) in enumerate(ORDER):
        tasks[TASKS[which]](*args)
        started += [n] * (len(sent) - len(started))
        while settled < len(sent) and started[settled] < n - LAG:
            sent[settled].wait_send()
            settled += 1
        if TASKS[which] == "sum_round" and args[0] == last_round - 1:
            lax.fori_loop(0, PIECES, settle_down, 0)
            lax.fori_loop(0, early_pieces, settle_sum, 0)
            for q in range(CHUNKS):
                @pl.when(active)
                def _():
                    side_copy(q).wait_send()

    for one in sent[settled:]:
        one.wait_send()
    lax.fori_loop(early_pieces, PIECES, settle_sum, 0)


TASKS = (
    "gather_own",
    "prepare",
    "gather_first",
    "gather_opposite",
    "gather_forward",
    "gather_last",
    "gather_done",
    "z_start",
    "upper",
    "z_round",
    "hand_over",
    "take_over",
    "sum_round",
    "lower",
    "scatter_partner",
    "scatter_far",
    "scatter_near",
    "scatter_column",
    "scatter_row",
    "scatter_done",
    "finish",
)
ORDER = (
    (0, 0), (1,), (2, 0), (0, 1), (3, 0), (4, 0, 0), (4, 0, 1), (4, 0, 2), (2, 1), (4, 0, 3), (4, 1, 0),
    (0, 2), (3, 1), (5, 0), (2, 2), (4, 1, 2), (4, 1, 1), (4, 1, 3), (6, 0), (7, 0), (8, 0, 0), (0, 3),
    (3, 2), (8, 0, 1), (4, 2, 0), (9, 0), (9, 1), (10, 0), (4, 2, 1), (5, 1), (11, 0), (9, 2), (2, 3),
    (12, 0), (9, 3), (4, 2, 3), (12, 1), (4, 2, 2), (6, 1), (9, 4), (8, 1, 0), (12, 2), (9, 5), (9, 6),
    (7, 1), (8, 1, 1), (12, 3), (12, 4), (3, 3), (4, 3, 0), (4, 3, 2), (9, 7), (4, 3, 1), (10, 1), (9, 8),
    (12, 5), (5, 2), (9, 9), (12, 6), (9, 10), (12, 7), (9, 11), (6, 2), (11, 1), (12, 8), (9, 12), (4, 3, 3),
    (8, 2, 0), (9, 13), (12, 9), (12, 10), (7, 2), (8, 2, 1), (9, 14), (12, 11), (5, 3), (9, 15), (9, 16),
    (12, 12), (10, 2), (6, 3), (12, 13), (9, 17), (7, 3), (8, 3, 0), (9, 18), (12, 14), (9, 19), (11, 2),
    (12, 15), (13, 0, 0), (12, 16), (14, 0, 0), (9, 20), (9, 21), (8, 3, 1), (12, 17), (9, 22), (12, 18),
    (13, 0, 1), (14, 0, 1), (9, 23), (12, 19), (15, 0, 0), (9, 24), (10, 3), (9, 25), (12, 20), (15, 0, 1),
    (9, 26), (12, 21), (16, 0, 0), (12, 22), (9, 27), (13, 1, 0), (9, 28), (14, 1, 0), (12, 23), (11, 3),
    (9, 29), (16, 0, 1), (12, 24), (13, 1, 1), (9, 30), (15, 1, 0), (14, 1, 1), (9, 31), (12, 25), (17, 0, 0),
    (9, 32), (12, 26), (9, 33), (12, 27), (15, 1, 1), (9, 34), (16, 1, 0), (12, 28), (17, 0, 1), (9, 35),
    (13, 2, 0), (9, 36), (18, 0, 0), (12, 29), (14, 2, 0), (12, 30), (16, 1, 1), (9, 37), (13, 2, 1),
    (14, 2, 1), (9, 38), (15, 2, 0), (9, 39), (12, 31), (12, 32), (17, 1, 0), (18, 0, 1), (9, 40), (12, 33),
    (15, 2, 1), (17, 1, 1), (9, 41), (12, 34), (9, 42), (16, 2, 0), (9, 43), (12, 35), (13, 3, 0), (14, 3, 0),
    (12, 36), (18, 1, 0), (16, 2, 1), (13, 3, 1), (12, 37), (14, 3, 1), (12, 38), (15, 3, 0), (15, 3, 1),
    (18, 1, 1), (19, 1, 0), (17, 2, 0), (12, 39), (19, 0, 1), (19, 0, 0), (12, 40), (17, 2, 1), (12, 41),
    (16, 3, 0), (16, 3, 1), (12, 42), (12, 43), (18, 2, 1), (12, 44), (17, 3, 0), (17, 3, 1), (18, 2, 0),
    (12, 45), (12, 46), (18, 3, 0), (18, 3, 1), (19, 2, 0), (19, 2, 1), (19, 1, 1), (20, 1), (20, 0),
    (19, 3, 0), (20, 2), (19, 3, 1), (20, 3),
)


def per_device(upstream, input_panel):
    f32, bf16 = jnp.float32, jnp.bfloat16
    total = CHUNKS * WIDE
    vmem = pltpu.VMEM
    result = pl.pallas_call(
        kernel,
        out_shape=jax.ShapeDtypeStruct((32, ROWS), f32),
        in_specs=[pl.BlockSpec(memory_space=pl.ANY), pl.BlockSpec(memory_space=pltpu.VMEM)],
        out_specs=pl.BlockSpec(memory_space=pltpu.VMEM),
        scratch_shapes=[
            vmem((total, ROWS), f32),
            vmem((total, COLS), f32),
            vmem((total, COLS), f32),
            vmem((total, COLS), f32),
            vmem((2 * total, COLS), f32),
            vmem((total, ROWS), f32),
            vmem((total // 2, ROWS), f32),
            vmem((CHUNKS * 64, HALF), f32),
            vmem((CHUNKS * 64, ROWS), f32),
            vmem((CHUNKS * 16, HALF), f32),
            vmem((CHUNKS * 16, ROWS), f32),
            vmem((CHUNKS * 8, ROWS), f32),
            vmem((ROWS, COLS), f32),
            vmem((ROWS, COLS), bf16),
            vmem((ROWS, COLS), bf16),
            vmem((WIDE, ROWS), bf16),
            vmem((WIDE, ROWS), bf16),
            vmem((WIDE, COLS), bf16),
            vmem((WIDE, COLS), bf16),
            pltpu.SemaphoreType.DMA((COPIES,)),
            pltpu.SemaphoreType.DMA((COPIES,)),
            pltpu.SemaphoreType.DMA((3 * PIECES,)),
            pltpu.SemaphoreType.DMA((PIECES,)),
            pltpu.SemaphoreType.DMA((2 * PIECES,)),
            pltpu.SemaphoreType.DMA((PIECES * PART // 8,)),
            pltpu.SemaphoreType.DMA((CHUNKS * 4,)),
            pltpu.SemaphoreType.DMA((CHUNKS,)),
            pltpu.SemaphoreType.DMA((CHUNKS,)),
            pltpu.SemaphoreType.DMA((8,)),
        ],
        compiler_params=pltpu.CompilerParams(
            collective_id=0, has_side_effects=True, vmem_limit_bytes=60 * 1024 * 1024
        ),
    )(upstream, input_panel.T)
    return result.T


def solution(mesh):
    placed = (P("row", ("col", "rep")), P("row", ("col", "rep")))
    return jax.shard_map(
        per_device, mesh=mesh, in_specs=placed, out_specs=P("row", ("col", "rep")), check_vma=False
    )
```
